128 devices in a mesh: ty: 2 (over core), tx: 64 (over z, y, x).
Axes of the slice: x: 4, y: 4, z: 4, core: 2. Of those that a mesh axis runs over, the one named last changes fastest.
Arguments:
- w_one: float32 [64, 2, 6, 128, 512], P('tx', 'ty')
- w_two: float32 [64, 2, 6, 512, 128], P('tx', 'ty')
- inputs: bfloat16 [64, 2, 8, 1024, 128], P('tx', 'ty')
- targets: bfloat16 [64, 2, 8, 1024, 128], P('tx', 'ty')
Outputs:
- output 1: float32 [64, 2, 6, 128, 512], P('tx', 'ty')
- output 2: float32 [64, 2, 6, 512, 128], P('tx', 'ty')
- output 3: float32 [64, 2, 8], P('tx', 'ty')
All inputs are finite; a program needn't handle non-finite values.
Results may differ from the reference program's by a relative error of at most 0.00442233.
Values are sent between devices in bfloat16 or wider.
A program may use at most 1 GiB of HBM per device.

```python
import jax
import jax.numpy as jnp
from jax import lax

MODEL_WIDTH = 128
FFN_WIDTH = 512
LAYERS = 6
NUM_STEPS = 8
LOCAL_ROWS = 1024
GRID_X = 64
GRID_Y = 2
NORM_EPS = 1e-6
LEARN_RATE = MODEL_WIDTH / (FFN_WIDTH * LAYERS)
REPLICAS = GRID_X * GRID_Y


def setup_inputs(seed: int = 0) -> dict:
    key_list = jax.random.split(jax.random.key(seed), 8)
    base_one = jax.random.normal(key_list[0], (LAYERS, MODEL_WIDTH, FFN_WIDTH), jnp.float32)
    own_one = jax.random.normal(key_list[1], (GRID_X, GRID_Y, LAYERS, MODEL_WIDTH, FFN_WIDTH), jnp.float32)
    base_two = jax.random.normal(key_list[2], (LAYERS, FFN_WIDTH, MODEL_WIDTH), jnp.float32)
    own_two = jax.random.normal(key_list[3], (GRID_X, GRID_Y, LAYERS, FFN_WIDTH, MODEL_WIDTH), jnp.float32)
    w_one = (base_one + 0.6 * own_one) * MODEL_WIDTH ** -0.5
    w_two = (base_two + 0.6 * own_two) * FFN_WIDTH ** -0.5
    data_shape = (GRID_X, GRID_Y, NUM_STEPS, LOCAL_ROWS, MODEL_WIDTH)
    scale_shape = (GRID_X, GRID_Y, NUM_STEPS, 1, 1)
    input_scale = jnp.exp2(jax.random.uniform(key_list[4], scale_shape, jnp.float32, -1.0, 1.0))
    target_scale = jnp.exp2(jax.random.uniform(key_list[5], scale_shape, jnp.float32, -1.0, 1.0))
    inputs = (jax.random.normal(key_list[6], data_shape, jnp.float32) * input_scale).astype(jnp.bfloat16)
    targets = (jax.random.normal(key_list[7], data_shape, jnp.float32) * target_scale).astype(jnp.bfloat16)
    return {"w_one": w_one, "w_two": w_two, "inputs": inputs, "targets": targets}


def rms_norm(hidden):
    hid_f = hidden.astype(jnp.float32)
    inv_rms = lax.rsqrt(jnp.mean(hid_f * hid_f, axis=-1, keepdims=True) + NORM_EPS)
    return (hid_f * inv_rms).astype(jnp.bfloat16)


def replica_loss(w_one, w_two, step_acts, step_goals):
    def layer_fn(hidden, weights):
        layer_one, layer_two = weights
        normed = rms_norm(hidden)
        pre_act = jnp.dot(normed, layer_one.astype(jnp.bfloat16), preferred_element_type=jnp.float32)
        hidden_act = jax.nn.gelu(pre_act).astype(jnp.bfloat16)
        mlp_out = jnp.dot(hidden_act, layer_two.astype(jnp.bfloat16), preferred_element_type=jnp.float32)
        return (hidden.astype(jnp.float32) + mlp_out).astype(jnp.bfloat16), None

    final_h, _ = lax.scan(layer_fn, step_acts, (w_one, w_two))
    error_term = final_h.astype(jnp.float32) - step_goals.astype(jnp.float32)
    return jnp.mean(error_term * error_term)


def gossip_mix(params):
    sent_copy = params.astype(jnp.bfloat16).astype(jnp.float32)
    mix_sum = params + jnp.roll(sent_copy, 1, axis=0)
    mix_sum = mix_sum + jnp.roll(sent_copy, -1, axis=0)
    mix_sum = mix_sum + jnp.roll(sent_copy, 1, axis=1)
    mix_sum = mix_sum + jnp.roll(sent_copy, -1, axis=1)
    return mix_sum / 5.0


def reference(w_one, w_two, inputs, targets):
    value_grad_fn = jax.value_and_grad(replica_loss, argnums=(0, 1))

    def replica_grads(operands):
        return value_grad_fn(operands[0], operands[1], operands[2], operands[3])

    def step_fn(params, step_batch):
        p_one, p_two = params
        step_acts, step_goals = step_batch
        flat_args = (
            p_one.reshape((REPLICAS,) + p_one.shape[2:]),
            p_two.reshape((REPLICAS,) + p_two.shape[2:]),
            step_acts.reshape((REPLICAS,) + step_acts.shape[2:]),
            step_goals.reshape((REPLICAS,) + step_goals.shape[2:]),
        )
        loss_vals, grad_pair = lax.map(replica_grads, flat_args)
        new_one = gossip_mix(p_one) - LEARN_RATE * grad_pair[0].reshape(p_one.shape)
        new_two = gossip_mix(p_two) - LEARN_RATE * grad_pair[1].reshape(p_two.shape)
        return (new_one, new_two), loss_vals.reshape(GRID_X, GRID_Y)

    step_data = (jnp.moveaxis(inputs, 2, 0), jnp.moveaxis(targets, 2, 0))
    final_pair, step_losses = lax.scan(step_fn, (w_one, w_two), step_data)
    return final_pair[0], final_pair[1], jnp.moveaxis(step_losses, 0, 2)
```

```python
import functools

import jax
import jax.numpy as jnp
from jax import lax
from jax.experimental import pallas as pl
from jax.experimental.pallas import tpu as pltpu
from jax.sharding import PartitionSpec as P

NORM_EPS = 1e-6
GELU_SCALE = 0.7978845608028654
GELU_CUBIC = 0.044715
MESH = pl.DeviceIdType.MESH
BF16 = jnp.bfloat16
F32 = jnp.float32


def dot(lhs, rhs, lhs_dim, rhs_dim):
    return lax.dot_general(lhs, rhs, (((lhs_dim,), (rhs_dim,)), ((), ())), preferred_element_type=F32)


def train_kernel(
    dims,
    w_one, w_two, inputs, targets,
    out_one, out_two, losses,
    master, copies, recv, hidden, normed, inv_rms, act, slope, d_hid, d_pre, goals, stage,
    load_sem, data_sem, send_sem, recv_sem, out_sem,
):
    grid_x, steps, layers, rows, width, ffn, block = dims
    learn_rate = width / (ffn * layers)
    blocks = [pl.ds(start, block) for start in range(0, rows, block)]
    me_x = lax.axis_index("tx")
    me_y = lax.axis_index("ty")
    next_x = lax.rem(me_x + 1, grid_x)
    prev_x = lax.rem(me_x + grid_x - 1, grid_x)
    peers = ({"tx": next_x}, {"tx": prev_x}, {"ty": 1 - me_y})

    def load_copies(layer):
        return (
            pltpu.make_async_copy(w_one.at[layer], master.at[layer, pl.ds(0, width)], load_sem.at[0, layer]),
            pltpu.make_async_copy(w_two.at[layer], stage.at[layer], load_sem.at[1, layer]),
        )

    def out_copies(layer):
        return (
            pltpu.make_async_copy(master.at[layer, pl.ds(0, width)], out_one.at[layer], out_sem.at[0, layer]),
            pltpu.make_async_copy(stage.at[layer], out_two.at[layer], out_sem.at[1, layer]),
        )

    def acts_copy(step):
        return pltpu.make_async_copy(inputs.at[step], hidden.at[0], data_sem.at[0])

    def goals_copy(step):
        return pltpu.make_async_copy(targets.at[step], goals, data_sem.at[1])

    def sends(slot, layer):
        return [
            pltpu.make_async_remote_copy(
                src_ref=copies.at[slot, layer],
                dst_ref=recv.at[peer_idx, slot, layer],
                send_sem=send_sem.at[peer_idx, slot, layer],
                recv_sem=recv_sem.at[peer_idx, slot, layer],
                device_id=peer,
                device_id_type=MESH,
            )
            for peer_idx, peer in enumerate(peers)
        ]

    for layer in reversed(range(layers)):
        for copy in load_copies(layer):
            copy.start()
    acts_copy(0).start()
    goals_copy(0).start()

    barrier = pltpu.get_barrier_semaphore()
    for peer in peers:
        pl.semaphore_signal(barrier, inc=1, device_id=peer, device_id_type=MESH)
    pl.semaphore_wait(barrier, 3)

    def first_body(idx, carry):
        layer = layers - 1 - idx
        for copy in load_copies(layer):
            copy.wait()
        copies[0, layer, :width, :] = master[layer, :width, :].astype(BF16)
        turned = stage[layer].T
        master[layer, width:, :] = turned
        copies[0, layer, width:, :] = turned.astype(BF16)
        for copy in sends(0, layer):
            copy.start()
        return carry

    lax.fori_loop(0, layers, first_body, 0)

    def step_body(step, carry):
        slot = lax.rem(step, 2)
        later = 1 - slot
        acts_copy(step).wait()

        def forward_body(layer, inner):
            cast_one = copies[slot, layer, :width, :]
            cast_two = copies[slot, layer, width:, :]
            for rows_ds in blocks:
                hid_f = hidden[layer, rows_ds, :].astype(F32)
                inv = lax.rsqrt(jnp.mean(hid_f * hid_f, axis=-1, keepdims=True) + NORM_EPS)
                inv = jnp.broadcast_to(inv, hid_f.shape)
                normed_b = (hid_f * inv).astype(BF16)
                inv_rms[layer, rows_ds, :] = inv
                normed[layer, rows_ds, :] = normed_b
                pre = dot(normed_b, cast_one, 1, 0)
                square = pre * pre
                tanh_v = jnp.tanh(pre * (GELU_SCALE + (GELU_SCALE * GELU_CUBIC) * square))
                cdf = 0.5 + 0.5 * tanh_v
                act_b = (pre * cdf).astype(BF16)
                act[layer, rows_ds, :] = act_b
                inner_slope = 0.5 * GELU_SCALE + (1.5 * GELU_SCALE * GELU_CUBIC) * square
                slope[layer, rows_ds, :] = cdf + (pre * inner_slope) * (1.0 - tanh_v * tanh_v)
                mlp_out = dot(act_b, cast_two, 1, 1)
                hidden[layer + 1, rows_ds, :] = (hid_f + mlp_out).astype(BF16)
            return inner

        lax.fori_loop(0, layers, forward_body, 0)

        @pl.when(step + 1 < steps)
        def _():
            acts_copy(step + 1).start()

        goals_copy(step).wait()
        total = jnp.zeros((8, width), F32)
        for rows_ds in blocks:
            error_term = hidden[layers, rows_ds, :].astype(F32) - goals[rows_ds, :].astype(F32)
            d_hid[rows_ds, :] = (error_term * (2.0 / (rows * width))).astype(BF16)
            total = total + jnp.sum((error_term * error_term).reshape(block // 8, 8, width), axis=0)
        losses[step] = jnp.sum(total) / (rows * width)

        @pl.when(step + 1 < steps)
        def _():
            goals_copy(step + 1).start()

        def backward_body(idx, inner):
            layer = layers - 1 - idx
            cast_two = copies[slot, layer, width:, :]
            for rows_ds in blocks:
                d_act = dot(d_hid[rows_ds, :], cast_two, 1, 0).astype(BF16).astype(F32)
                d_pre[rows_ds, :] = (d_act * slope[layer, rows_ds, :]).astype(BF16)
            grad_two = dot(d_hid[...], act[layer], 0, 0).astype(BF16)
            grad_one = dot(normed[layer], d_pre[...], 0, 0).astype(BF16)

            for copy in sends(slot, layer):
                copy.wait_recv()

            @pl.when(step > 0)
            def _():
                for copy in sends(later, layer):
                    copy.wait_send()

            for start, grad in ((0, grad_one), (width, grad_two)):
                part = pl.ds(start, width)
                other = recv[2, slot, layer, part, :].astype(F32)
                mixed = master[layer, part, :] + recv[0, slot, layer, part, :].astype(F32)
                mixed = mixed + recv[1, slot, layer, part, :].astype(F32)
                mixed = mixed + other
                mixed = mixed + other
                fresh = mixed * 0.2 - learn_rate * grad.astype(F32)
                master[layer, part, :] = fresh
                copies[later, layer, part, :] = fresh.astype(BF16)

            @pl.when(layer > 0)
            def _():
                cast_one = copies[slot, layer, :width, :]
                for rows_ds in blocks:
                    d_normed = dot(d_pre[rows_ds, :], cast_one, 1, 1).astype(BF16).astype(F32)
                    inv = inv_rms[layer, rows_ds, :]
                    normed_f = hidden[layer, rows_ds, :].astype(F32) * inv
                    along = jnp.mean(d_normed * normed_f, axis=-1, keepdims=True)
                    d_in = inv * (d_normed - normed_f * along)
                    d_hid[rows_ds, :] = (d_hid[rows_ds, :].astype(F32) + d_in).astype(BF16)

            @pl.when(step + 1 < steps)
            def _():
                for copy in sends(later, layer):
                    copy.start()

            @pl.when(step + 1 == steps)
            def _():
                stage[layer] = master[layer, width:, :].T
                for copy in out_copies(layer):
                    copy.start()

            return inner

        lax.fori_loop(0, layers, backward_body, 0)
        return carry

    lax.fori_loop(0, steps, step_body, 0)

    def last_body(layer, carry):
        for copy in sends((steps - 1) % 2, layer):
            copy.wait_send()
        for copy in out_copies(layer):
            copy.wait()
        return carry

    lax.fori_loop(0, layers, last_body, 0)


def solution(mesh):
    grid_x = mesh.shape["tx"]

    def device_train(w_one, w_two, inputs, targets):
        layers, width, ffn = w_one.shape[2:]
        steps, rows = inputs.shape[2:4]
        block = min(256, rows)
        dims = (grid_x, steps, layers, rows, width, ffn, block)
        any_spec = pl.BlockSpec(memory_space=pl.ANY)
        out_one, out_two, losses = pl.pallas_call(
            functools.partial(train_kernel, dims),
            out_shape=(
                jax.ShapeDtypeStruct((layers, width, ffn), F32),
                jax.ShapeDtypeStruct((layers, ffn, width), F32),
                jax.ShapeDtypeStruct((steps,), F32),
            ),
            in_specs=[any_spec] * 4,
            out_specs=(any_spec, any_spec, pl.BlockSpec(memory_space=pltpu.SMEM)),
            scratch_shapes=[
                pltpu.VMEM((layers, 2 * width, ffn), F32),
                pltpu.VMEM((2, layers, 2 * width, ffn), BF16),
                pltpu.VMEM((3, 2, layers, 2 * width, ffn), BF16),
                pltpu.VMEM((layers + 1, rows, width), BF16),
                pltpu.VMEM((layers, rows, width), BF16),
                pltpu.VMEM((layers, rows, width), F32),
                pltpu.VMEM((layers, rows, ffn), BF16),
                pltpu.VMEM((layers, rows, ffn), F32),
                pltpu.VMEM((rows, width), BF16),
                pltpu.VMEM((rows, ffn), BF16),
                pltpu.VMEM((rows, width), BF16),
                pltpu.VMEM((layers, ffn, width), F32),
                pltpu.SemaphoreType.DMA((2, layers)),
                pltpu.SemaphoreType.DMA((2,)),
                pltpu.SemaphoreType.DMA((3, 2, layers)),
                pltpu.SemaphoreType.DMA((3, 2, layers)),
                pltpu.SemaphoreType.DMA((2, layers)),
            ],
            compiler_params=pltpu.CompilerParams(
                collective_id=0, has_side_effects=True, vmem_limit_bytes=62 * 1024 * 1024
            ),
            name="gossip_train",
        )(w_one[0, 0], w_two[0, 0], inputs[0, 0], targets[0, 0])
        return out_one[None, None], out_two[None, None], losses[None, None]

    grid_spec = P("tx", "ty")
    return jax.shard_map(
        device_train,
        mesh=mesh,
        in_specs=(grid_spec, grid_spec, grid_spec, grid_spec),
        out_specs=(grid_spec, grid_spec, grid_spec),
        check_vma=False,
    )
```

```python
import functools

import jax
import jax.numpy as jnp
from jax import lax
from jax.experimental import pallas as pl
from jax.experimental.pallas import tpu as pltpu
from jax.sharding import PartitionSpec as P

NORM_EPS = 1e-6
GELU_SCALE = 0.7978845608028654
GELU_CUBIC = 0.044715
MESH = pl.DeviceIdType.MESH
BF16 = jnp.bfloat16
F32 = jnp.float32


def dot(lhs, rhs, lhs_dim, rhs_dim):
    return lax.dot_general(lhs, rhs, (((lhs_dim,), (rhs_dim,)), ((), ())), preferred_element_type=F32)


def train_kernel(
    dims,
    w_one, w_two, inputs, targets,
    master_one, stage, losses,
    master_two, copies, recv, hidden, normed, inv_rms, act, slope, d_hid, d_pre, goals,
    load_sem, data_sem, send_sem, recv_sem, entry_sem,
):
    grid_x, steps, layers, rows, width, ffn, block = dims
    learn_rate = width / (ffn * layers)
    blocks = [pl.ds(start, block) for start in range(0, rows, block)]
    me_x = lax.axis_index("tx")
    me_y = lax.axis_index("ty")
    next_x = lax.rem(me_x + 1, grid_x)
    prev_x = lax.rem(me_x + grid_x - 1, grid_x)
    peers = ({"tx": next_x}, {"tx": prev_x}, {"ty": 1 - me_y})

    def load_copies(layer):
        return (
            pltpu.make_async_copy(w_one.at[layer], master_one.at[layer], load_sem.at[0, layer]),
            pltpu.make_async_copy(w_two.at[layer], stage.at[layer], load_sem.at[1, layer]),
        )

    def acts_copy(step):
        return pltpu.make_async_copy(inputs.at[step], hidden.at[0], data_sem.at[0])

    def goals_copy(step):
        return pltpu.make_async_copy(targets.at[step], goals, data_sem.at[1])

    def sends(slot, layer, peer_ids=(0, 1, 2)):
        return [
            pltpu.make_async_remote_copy(
                src_ref=copies.at[slot, layer],
                dst_ref=recv.at[peer_idx, slot, layer],
                send_sem=send_sem.at[peer_idx, slot, layer],
                recv_sem=recv_sem.at[peer_idx, slot, layer],
                device_id=peers[peer_idx],
                device_id_type=MESH,
            )
            for peer_idx in peer_ids
        ]

    def start_sends(slot, layer, peer_ids=(0, 1, 2)):
        for copy in sends(slot, layer, peer_ids):
            copy.start()

    is_first = me_x == 0
    is_last = me_x == grid_x - 1
    barrier = pltpu.get_barrier_semaphore()
    pl.semaphore_signal(barrier, inc=1, device_id=peers[1], device_id_type=MESH)
    pl.semaphore_signal(barrier, inc=1, device_id=peers[2], device_id_type=MESH)

    @pl.when(jnp.logical_not(is_last))
    def _():
        pl.semaphore_signal(barrier, inc=1, device_id=peers[0], device_id_type=MESH)

    for layer in reversed(range(layers)):
        for copy in load_copies(layer):
            copy.start()
    acts_copy(0).start()
    goals_copy(0).start()

    pl.semaphore_wait(barrier, jnp.where(is_first, 2, 3))

    @pl.when(is_last)
    def _():
        pl.semaphore_signal(entry_sem, inc=1, device_id=peers[0], device_id_type=MESH)

    def first_body(idx, carry):
        layer = layers - 1 - idx
        for copy in load_copies(layer):
            copy.wait()
        copies[0, layer, :width, :] = master_one[layer].astype(BF16)
        turned = stage[layer].T
        master_two[layer] = turned
        copies[0, layer, width:, :] = turned.astype(BF16)
        start_sends(0, layer, (0, 2))

        @pl.when(jnp.logical_not(is_first))
        def _():
            start_sends(0, layer, (1,))

        return carry

    lax.fori_loop(0, layers, first_body, 0)

    @pl.when(is_first)
    def _():
        pl.semaphore_wait(entry_sem, 1)

        def late_body(idx, carry):
            start_sends(0, layers - 1 - idx, (1,))
            return carry

        lax.fori_loop(0, layers, late_body, 0)

    losses[...] = jnp.zeros(losses.shape, F32)

    def step_body(step, carry):
        slot = lax.rem(step, 2)
        later = 1 - slot
        acts_copy(step).wait()

        def forward_body(layer, inner):
            cast_one = copies[slot, layer, :width, :]
            cast_two = copies[slot, layer, width:, :]
            for rows_ds in blocks:
                hid_f = hidden[layer, rows_ds, :].astype(F32)
                inv = lax.rsqrt(jnp.mean(hid_f * hid_f, axis=-1, keepdims=True) + NORM_EPS)
                inv = jnp.broadcast_to(inv, hid_f.shape)
                normed_b = (hid_f * inv).astype(BF16)
                inv_rms[layer, rows_ds, :] = inv
                normed[layer, rows_ds, :] = normed_b
                pre = dot(normed_b, cast_one, 1, 0)
                square = pre * pre
                tanh_v = jnp.tanh(pre * (GELU_SCALE + (GELU_SCALE * GELU_CUBIC) * square))
                cdf = 0.5 + 0.5 * tanh_v
                act_b = (pre * cdf).astype(BF16)
                act[layer, rows_ds, :] = act_b
                inner_slope = 0.5 * GELU_SCALE + (1.5 * GELU_SCALE * GELU_CUBIC) * square
                slope[layer, rows_ds, :] = cdf + (pre * inner_slope) * (1.0 - tanh_v * tanh_v)
                mlp_out = dot(act_b, cast_two, 1, 1)
                hidden[layer + 1, rows_ds, :] = (hid_f + mlp_out).astype(BF16)
            return inner

        lax.fori_loop(0, layers, forward_body, 0)

        @pl.when(step + 1 < steps)
        def _():
            acts_copy(step + 1).start()

        goals_copy(step).wait()
        total = jnp.zeros((8, width), F32)
        for rows_ds in blocks:
            error_term = hidden[layers, rows_ds, :].astype(F32) - goals[rows_ds, :].astype(F32)
            d_hid[rows_ds, :] = (error_term * (2.0 / (rows * width))).astype(BF16)
            total = total + jnp.sum((error_term * error_term).reshape(block // 8, 8, width), axis=0)
        step_loss = jnp.sum(total) / (rows * width)
        lane = lax.broadcasted_iota(jnp.int32, losses.shape, 1)
        losses[...] = jnp.where(lane == step, step_loss, losses[...])

        @pl.when(step + 1 < steps)
        def _():
            goals_copy(step + 1).start()

        def backward_body(idx, inner):
            layer = layers - 1 - idx
            cast_two = copies[slot, layer, width:, :]
            for rows_ds in blocks:
                d_act = dot(d_hid[rows_ds, :], cast_two, 1, 0).astype(BF16).astype(F32)
                d_pre[rows_ds, :] = (d_act * slope[layer, rows_ds, :]).astype(BF16)
            grad_two = dot(d_hid[...], act[layer], 0, 0).astype(BF16)
            grad_one = dot(normed[layer], d_pre[...], 0, 0).astype(BF16)

            for copy in sends(slot, layer):
                copy.wait_recv()

            @pl.when(step > 0)
            def _():
                for copy in sends(later, layer):
                    copy.wait_send()

            for start, grad, master in ((0, grad_one, master_one), (width, grad_two, master_two)):
                part = pl.ds(start, width)
                other = recv[2, slot, layer, part, :].astype(F32)
                mixed = master[layer] + recv[0, slot, layer, part, :].astype(F32)
                mixed = mixed + recv[1, slot, layer, part, :].astype(F32)
                mixed = mixed + other
                mixed = mixed + other
                fresh = mixed * 0.2 - learn_rate * grad.astype(F32)
                master[layer] = fresh
                copies[later, layer, part, :] = fresh.astype(BF16)

            @pl.when(layer > 0)
            def _():
                cast_one = copies[slot, layer, :width, :]
                for rows_ds in blocks:
                    d_normed = dot(d_pre[rows_ds, :], cast_one, 1, 1).astype(BF16).astype(F32)
                    inv = inv_rms[layer, rows_ds, :]
                    normed_f = hidden[layer, rows_ds, :].astype(F32) * inv
                    along = jnp.mean(d_normed * normed_f, axis=-1, keepdims=True)
                    d_in = inv * (d_normed - normed_f * along)
                    d_hid[rows_ds, :] = (d_hid[rows_ds, :].astype(F32) + d_in).astype(BF16)

            @pl.when(step + 1 < steps)
            def _():
                start_sends(later, layer)

            @pl.when(step + 1 == steps)
            def _():
                stage[layer] = master_two[layer].T

            return inner

        lax.fori_loop(0, layers, backward_body, 0)
        return carry

    lax.fori_loop(0, steps, step_body, 0)

    def last_body(layer, carry):
        for copy in sends((steps - 1) % 2, layer):
            copy.wait_send()
        return carry

    lax.fori_loop(0, layers, last_body, 0)


def write_kernel(one, two, losses, out_one, out_two, out_losses, sems):
    copies = [
        pltpu.make_async_copy(src, dst, sems.at[idx])
        for idx, (src, dst) in enumerate(((one, out_one), (two, out_two), (losses, out_losses)))
    ]
    for copy in copies:
        copy.start()
    for copy in copies:
        copy.wait()


def solution(mesh):
    grid_x = mesh.shape["tx"]

    def device_train(w_one, w_two, inputs, targets):
        layers, width, ffn = w_one.shape[2:]
        steps, rows = inputs.shape[2:4]
        block = min(256, rows)
        dims = (grid_x, steps, layers, rows, width, ffn, block)
        any_spec = pl.BlockSpec(memory_space=pl.ANY)
        vmem_spec = pl.BlockSpec(memory_space=pltpu.VMEM)
        shapes = ((layers, width, ffn), (layers, ffn, width), (1, steps))
        one, two, losses = pl.pallas_call(
            functools.partial(train_kernel, dims),
            out_shape=tuple(pltpu.VMEM(shape, F32) for shape in shapes),
            in_specs=[any_spec] * 4,
            out_specs=(vmem_spec,) * 3,
            scratch_shapes=[
                pltpu.VMEM((layers, width, ffn), F32),
                pltpu.VMEM((2, layers, 2 * width, ffn), BF16),
                pltpu.VMEM((3, 2, layers, 2 * width, ffn), BF16),
                pltpu.VMEM((layers + 1, rows, width), BF16),
                pltpu.VMEM((layers, rows, width), BF16),
                pltpu.VMEM((layers, rows, width), F32),
                pltpu.VMEM((layers, rows, ffn), BF16),
                pltpu.VMEM((layers, rows, ffn), F32),
                pltpu.VMEM((rows, width), BF16),
                pltpu.VMEM((rows, ffn), BF16),
                pltpu.VMEM((rows, width), BF16),
                pltpu.SemaphoreType.DMA((2, layers)),
                pltpu.SemaphoreType.DMA((2,)),
                pltpu.SemaphoreType.DMA((3, 2, layers)),
                pltpu.SemaphoreType.DMA((3, 2, layers)),
                pltpu.SemaphoreType.REGULAR,
            ],
            compiler_params=pltpu.CompilerParams(
                collective_id=0, has_side_effects=True, vmem_limit_bytes=52 * 1024 * 1024
            ),
            name="gossip_train",
        )(w_one[0, 0], w_two[0, 0], inputs[0, 0], targets[0, 0])
        out_one, out_two, out_losses = pl.pallas_call(
            write_kernel,
            out_shape=tuple(jax.ShapeDtypeStruct(shape, F32) for shape in shapes),
            in_specs=[vmem_spec] * 3,
            out_specs=(any_spec,) * 3,
            scratch_shapes=[pltpu.SemaphoreType.DMA((3,))],
            compiler_params=pltpu.CompilerParams(vmem_limit_bytes=1024 * 1024),
            name="write_out",
        )(one, two, losses)
        return out_one[None, None], out_two[None, None], out_losses[None]

    grid_spec = P("tx", "ty")
    return jax.shard_map(
        device_train,
        mesh=mesh,
        in_specs=(grid_spec, grid_spec, grid_spec, grid_spec),
        out_specs=(grid_spec, grid_spec, grid_spec),
        check_vma=False,
    )
```

```python
import functools

import jax
import jax.numpy as jnp
from jax import lax
from jax.experimental import pallas as pl
from jax.experimental.pallas import tpu as pltpu
from jax.sharding import PartitionSpec as P

NORM_EPS = 1e-6
GELU_SCALE = 0.7978845608028654
GELU_CUBIC = 0.044715
MESH = pl.DeviceIdType.MESH
BF16 = jnp.bfloat16
F32 = jnp.float32


def dot(lhs, rhs, lhs_dim, rhs_dim):
    return lax.dot_general(lhs, rhs, (((lhs_dim,), (rhs_dim,)), ((), ())), preferred_element_type=F32)


def train_kernel(
    dims,
    w_one, w_two, inputs, targets,
    master_one, stage, losses,
    master_two, copies, recv, hidden, normed, inv_rms, act, slope, d_hid, d_pre, goals, relay,
    load_sem, data_sem, send_sem, recv_sem, relay_sem, entry_sem,
):
    grid_x, steps, layers, rows, width, ffn, block = dims
    learn_rate = width / (ffn * layers)
    blocks = [pl.ds(start, block) for start in range(0, rows, block)]
    me_x = lax.axis_index("tx")
    me_y = lax.axis_index("ty")
    next_x = lax.rem(me_x + 1, grid_x)
    prev_x = lax.rem(me_x + grid_x - 1, grid_x)
    peers = ({"tx": next_x}, {"tx": prev_x}, {"ty": 1 - me_y})

    def load_copies(layer):
        return (
            pltpu.make_async_copy(w_one.at[layer], master_one.at[layer], load_sem.at[0, layer]),
            pltpu.make_async_copy(w_two.at[layer], stage.at[layer], load_sem.at[1, layer]),
        )

    def acts_copy(step):
        return pltpu.make_async_copy(inputs.at[step], hidden.at[0], data_sem.at[0])

    def goals_copy(step):
        return pltpu.make_async_copy(targets.at[step], goals, data_sem.at[1])

    def sends(slot, layer, peer_ids=(0, 1, 2)):
        return [
            pltpu.make_async_remote_copy(
                src_ref=copies.at[slot, layer],
                dst_ref=recv.at[peer_idx, slot, layer],
                send_sem=send_sem.at[peer_idx, slot, layer],
                recv_sem=recv_sem.at[peer_idx, slot, layer],
                device_id=peers[peer_idx],
                device_id_type=MESH,
            )
            for peer_idx in peer_ids
        ]

    def start_sends(slot, layer, peer_ids=(0, 1, 2)):
        for copy in sends(slot, layer, peer_ids):
            copy.start()

    near, far = (4, 8) if grid_x >= 32 else (2, 3)
    offset = jnp.where(me_y == 0, near, far)
    first, last = 0, grid_x - 1
    low_relay, high_relay = first + offset, last - offset
    is_first, is_last = me_x == first, me_x == last
    is_low, is_high = me_x == low_relay, me_x == high_relay
    up_rows, down_rows = 3 * width // 2, width

    def at_x(index):
        return {"tx": index}

    def direct_part(peer_idx, start):
        part = pl.ds(start, 2 * width - start)
        return pltpu.make_async_remote_copy(
            src_ref=copies.at[0, 0, part],
            dst_ref=recv.at[peer_idx, 0, 0, part],
            send_sem=send_sem.at[peer_idx, 0, 0],
            recv_sem=recv_sem.at[peer_idx, 0, 0],
            device_id=peers[peer_idx],
            device_id_type=MESH,
        )

    def to_relay(peer_idx, size, index):
        return pltpu.make_async_remote_copy(
            src_ref=copies.at[0, 0, pl.ds(0, size)],
            dst_ref=relay.at[pl.ds(0, size)],
            send_sem=send_sem.at[peer_idx, 0, 0],
            recv_sem=relay_sem.at[0],
            device_id=at_x(index),
            device_id_type=MESH,
        )

    def from_relay(peer_idx, size, index):
        return pltpu.make_async_remote_copy(
            src_ref=relay.at[pl.ds(0, size)],
            dst_ref=recv.at[peer_idx, 0, 0, pl.ds(0, size)],
            send_sem=relay_sem.at[1],
            recv_sem=recv_sem.at[peer_idx, 0, 0],
            device_id=at_x(index),
            device_id_type=MESH,
        )

    def cast_layer(layer):
        for copy in load_copies(layer):
            copy.wait()
        copies[0, layer, :width, :] = master_one[layer].astype(BF16)
        turned = stage[layer].T
        master_two[layer] = turned
        copies[0, layer, width:, :] = turned.astype(BF16)

    def first_sends(layer):
        start_sends(0, layer, (2,))
        by_relay = jnp.logical_and(is_last, layer == 0)

        @pl.when(jnp.logical_not(by_relay))
        def _():
            start_sends(0, layer, (0,))

        @pl.when(by_relay)
        def _():
            to_relay(0, up_rows, high_relay).start()
            direct_part(0, up_rows).start()

        @pl.when(jnp.logical_not(is_first))
        def _():
            start_sends(0, layer, (1,))

    for copy in load_copies(layers - 1):
        copy.start()

    barrier = pltpu.get_barrier_semaphore()

    def announce(peer):
        pl.semaphore_signal(barrier, inc=1, device_id=peer, device_id_type=MESH)

    announce(peers[1])
    announce(peers[2])

    @pl.when(jnp.logical_not(is_last))
    def _():
        announce(peers[0])

    @pl.when(is_first)
    def _():
        announce(at_x(high_relay))

    @pl.when(is_low)
    def _():
        announce(at_x(first))
        announce(at_x(last))

    @pl.when(is_high)
    def _():
        announce(at_x(last))

    cast_layer(layers - 1)
    pl.semaphore_wait(barrier, 3 + 2 * is_last.astype(jnp.int32) + is_high.astype(jnp.int32))
    first_sends(layers - 1)

    for layer in reversed(range(layers - 1)):
        for copy in load_copies(layer):
            copy.start()
    acts_copy(0).start()
    goals_copy(0).start()

    @pl.when(is_last)
    def _():
        for index in (first, low_relay):
            pl.semaphore_signal(entry_sem, inc=1, device_id=at_x(index), device_id_type=MESH)

    def first_body(idx, carry):
        layer = layers - 1 - idx
        cast_layer(layer)
        first_sends(layer)
        return carry

    lax.fori_loop(1, layers, first_body, 0)

    @pl.when(is_first)
    def _():
        to_relay(1, down_rows, low_relay).start()
        pl.semaphore_wait(entry_sem, 1)

        def late_body(idx, carry):
            start_sends(0, layers - 1 - idx, (1,))
            return carry

        lax.fori_loop(0, layers - 1, late_body, 0)
        direct_part(1, down_rows).start()

    losses[...] = jnp.zeros(losses.shape, F32)

    def step_body(step, carry):
        slot = lax.rem(step, 2)
        later = 1 - slot
        acts_copy(step).wait()

        def forward_body(layer, inner):
            cast_one = copies[slot, layer, :width, :]
            cast_two = copies[slot, layer, width:, :]
            for rows_ds in blocks:
                hid_f = hidden[layer, rows_ds, :].astype(F32)
                inv = lax.rsqrt(jnp.mean(hid_f * hid_f, axis=-1, keepdims=True) + NORM_EPS)
                inv = jnp.broadcast_to(inv, hid_f.shape)
                normed_b = (hid_f * inv).astype(BF16)
                inv_rms[layer, rows_ds, :] = inv
                normed[layer, rows_ds, :] = normed_b
                pre = dot(normed_b, cast_one, 1, 0)
                square = pre * pre
                tanh_v = jnp.tanh(pre * (GELU_SCALE + (GELU_SCALE * GELU_CUBIC) * square))
                cdf = 0.5 + 0.5 * tanh_v
                act_b = (pre * cdf).astype(BF16)
                act[layer, rows_ds, :] = act_b
                inner_slope = 0.5 * GELU_SCALE + (1.5 * GELU_SCALE * GELU_CUBIC) * square
                slope[layer, rows_ds, :] = cdf + (pre * inner_slope) * (1.0 - tanh_v * tanh_v)
                mlp_out = dot(act_b, cast_two, 1, 1)
                hidden[layer + 1, rows_ds, :] = (hid_f + mlp_out).astype(BF16)
            return inner

        lax.fori_loop(0, layers, forward_body, 0)

        @pl.when(step + 1 < steps)
        def _():
            acts_copy(step + 1).start()

        @pl.when(jnp.logical_and(step == 0, is_high))
        def _():
            to_relay(0, up_rows, high_relay).wait_recv()
            from_relay(0, up_rows, first).start()

        @pl.when(jnp.logical_and(step == 0, is_low))
        def _():
            to_relay(1, down_rows, low_relay).wait_recv()
            pl.semaphore_wait(entry_sem, 1)
            from_relay(1, down_rows, last).start()

        goals_copy(step).wait()
        total = jnp.zeros((8, width), F32)
        for rows_ds in blocks:
            error_term = hidden[layers, rows_ds, :].astype(F32) - goals[rows_ds, :].astype(F32)
            d_hid[rows_ds, :] = (error_term * (2.0 / (rows * width))).astype(BF16)
            total = total + jnp.sum((error_term * error_term).reshape(block // 8, 8, width), axis=0)
        step_loss = jnp.sum(total) / (rows * width)
        lane = lax.broadcasted_iota(jnp.int32, losses.shape, 1)
        losses[...] = jnp.where(lane == step, step_loss, losses[...])

        @pl.when(step + 1 < steps)
        def _():
            goals_copy(step + 1).start()

        def backward_body(idx, inner):
            layer = layers - 1 - idx
            cast_two = copies[slot, layer, width:, :]
            for rows_ds in blocks:
                d_act = dot(d_hid[rows_ds, :], cast_two, 1, 0).astype(BF16).astype(F32)
                d_pre[rows_ds, :] = (d_act * slope[layer, rows_ds, :]).astype(BF16)
            grad_two = dot(d_hid[...], act[layer], 0, 0).astype(BF16)
            grad_one = dot(normed[layer], d_pre[...], 0, 0).astype(BF16)

            for copy in sends(slot, layer):
                copy.wait_recv()

            @pl.when(step > 0)
            def _():
                for copy in sends(later, layer):
                    copy.wait_send()

            for start, grad, master in ((0, grad_one, master_one), (width, grad_two, master_two)):
                part = pl.ds(start, width)
                other = recv[2, slot, layer, part, :].astype(F32)
                mixed = master[layer] + recv[0, slot, layer, part, :].astype(F32)
                mixed = mixed + recv[1, slot, layer, part, :].astype(F32)
                mixed = mixed + other
                mixed = mixed + other
                fresh = mixed * 0.2 - learn_rate * grad.astype(F32)
                master[layer] = fresh
                copies[later, layer, part, :] = fresh.astype(BF16)

            @pl.when(layer > 0)
            def _():
                cast_one = copies[slot, layer, :width, :]
                for rows_ds in blocks:
                    d_normed = dot(d_pre[rows_ds, :], cast_one, 1, 1).astype(BF16).astype(F32)
                    inv = inv_rms[layer, rows_ds, :]
                    normed_f = hidden[layer, rows_ds, :].astype(F32) * inv
                    along = jnp.mean(d_normed * normed_f, axis=-1, keepdims=True)
                    d_in = inv * (d_normed - normed_f * along)
                    d_hid[rows_ds, :] = (d_hid[rows_ds, :].astype(F32) + d_in).astype(BF16)

            @pl.when(step + 1 < steps)
            def _():
                start_sends(later, layer)

            @pl.when(step + 1 == steps)
            def _():
                stage[layer] = master_two[layer].T

            return inner

        lax.fori_loop(0, layers, backward_body, 0)
        return carry

    lax.fori_loop(0, steps, step_body, 0)

    def last_body(layer, carry):
        for copy in sends((steps - 1) % 2, layer):
            copy.wait_send()
        return carry

    lax.fori_loop(0, layers, last_body, 0)

    @pl.when(is_high)
    def _():
        from_relay(0, up_rows, first).wait_send()

    @pl.when(is_low)
    def _():
        from_relay(1, down_rows, last).wait_send()


def write_kernel(one, two, losses, out_one, out_two, out_losses, sems):
    copies = [
        pltpu.make_async_copy(src, dst, sems.at[idx])
        for idx, (src, dst) in enumerate(((one, out_one), (two, out_two), (losses, out_losses)))
    ]
    for copy in copies:
        copy.start()
    for copy in copies:
        copy.wait()


def solution(mesh):
    grid_x = mesh.shape["tx"]

    def device_train(w_one, w_two, inputs, targets):
        layers, width, ffn = w_one.shape[2:]
        steps, rows = inputs.shape[2:4]
        block = min(256, rows)
        dims = (grid_x, steps, layers, rows, width, ffn, block)
        any_spec = pl.BlockSpec(memory_space=pl.ANY)
        vmem_spec = pl.BlockSpec(memory_space=pltpu.VMEM)
        shapes = ((layers, width, ffn), (layers, ffn, width), (1, steps))
        one, two, losses = pl.pallas_call(
            functools.partial(train_kernel, dims),
            out_shape=tuple(pltpu.VMEM(shape, F32) for shape in shapes),
            in_specs=[any_spec] * 4,
            out_specs=(vmem_spec,) * 3,
            scratch_shapes=[
                pltpu.VMEM((layers, width, ffn), F32),
                pltpu.VMEM((2, layers, 2 * width, ffn), BF16),
                pltpu.VMEM((3, 2, layers, 2 * width, ffn), BF16),
                pltpu.VMEM((layers + 1, rows, width), BF16),
                pltpu.VMEM((layers, rows, width), BF16),
                pltpu.VMEM((layers, rows, width), F32),
                pltpu.VMEM((layers, rows, ffn), BF16),
                pltpu.VMEM((layers, rows, ffn), F32),
                pltpu.VMEM((rows, width), BF16),
                pltpu.VMEM((rows, ffn), BF16),
                pltpu.VMEM((rows, width), BF16),
                pltpu.VMEM((2 * width, ffn), BF16),
                pltpu.SemaphoreType.DMA((2, layers)),
                pltpu.SemaphoreType.DMA((2,)),
                pltpu.SemaphoreType.DMA((3, 2, layers)),
                pltpu.SemaphoreType.DMA((3, 2, layers)),
                pltpu.SemaphoreType.DMA((2,)),
                pltpu.SemaphoreType.REGULAR,
            ],
            compiler_params=pltpu.CompilerParams(
                collective_id=0, has_side_effects=True, vmem_limit_bytes=52 * 1024 * 1024
            ),
            name="gossip_train",
        )(w_one[0, 0], w_two[0, 0], inputs[0, 0], targets[0, 0])
        out_one, out_two, out_losses = pl.pallas_call(
            write_kernel,
            out_shape=tuple(jax.ShapeDtypeStruct(shape, F32) for shape in shapes),
            in_specs=[vmem_spec] * 3,
            out_specs=(any_spec,) * 3,
            scratch_shapes=[pltpu.SemaphoreType.DMA((3,))],
            compiler_params=pltpu.CompilerParams(vmem_limit_bytes=1024 * 1024),
            name="write_out",
        )(one, two, losses)
        return out_one[None, None], out_two[None, None], out_losses[None]

    grid_spec = P("tx", "ty")
    return jax.shard_map(
        device_train,
        mesh=mesh,
        in_specs=(grid_spec, grid_spec, grid_spec, grid_spec),
        out_specs=(grid_spec, grid_spec, grid_spec),
        check_vma=False,
    )
```

```python
import functools

import jax
import jax.numpy as jnp
from jax import lax
from jax.experimental import pallas as pl
from jax.experimental.pallas import tpu as pltpu
from jax.sharding import PartitionSpec as P

NORM_EPS = 1e-6
GELU_SCALE = 0.7978845608028654
GELU_CUBIC = 0.044715
MESH = pl.DeviceIdType.MESH
BF16 = jnp.bfloat16
F32 = jnp.float32


def dot(lhs, rhs, lhs_dim, rhs_dim):
    return lax.dot_general(lhs, rhs, (((lhs_dim,), (rhs_dim,)), ((), ())), preferred_element_type=F32)


def train_kernel(
    dims,
    w_one, w_two, inputs, targets,
    master_one, stage, losses,
    master_two, copies, recv, hidden, normed, inv_rms, act, slope, d_hid, d_pre, goals, relay,
    load_sem, data_sem, send_sem, recv_sem, relay_sem, entry_sem,
):
    grid_x, steps, layers, rows, width, ffn, block = dims
    learn_rate = width / (ffn * layers)
    blocks = [pl.ds(start, block) for start in range(0, rows, block)]
    me_x = lax.axis_index("tx")
    me_y = lax.axis_index("ty")
    next_x = lax.rem(me_x + 1, grid_x)
    prev_x = lax.rem(me_x + grid_x - 1, grid_x)
    peers = ({"tx": next_x}, {"tx": prev_x}, {"ty": 1 - me_y})

    def load_copies(layer):
        return (
            pltpu.make_async_copy(w_one.at[layer], master_one.at[layer], load_sem.at[0, layer]),
            pltpu.make_async_copy(w_two.at[layer], stage.at[layer], load_sem.at[1, layer]),
        )

    def acts_copy(step):
        return pltpu.make_async_copy(inputs.at[step], hidden.at[0], data_sem.at[0])

    def goals_copy(step):
        return pltpu.make_async_copy(targets.at[step], goals, data_sem.at[1])

    def sends(slot, layer, peer_ids=(0, 1, 2)):
        return [
            pltpu.make_async_remote_copy(
                src_ref=copies.at[slot, layer],
                dst_ref=recv.at[peer_idx, slot, layer],
                send_sem=send_sem.at[peer_idx, slot, layer],
                recv_sem=recv_sem.at[peer_idx, slot, layer],
                device_id=peers[peer_idx],
                device_id_type=MESH,
            )
            for peer_idx in peer_ids
        ]

    def start_sends(slot, layer, peer_ids=(0, 1, 2)):
        for copy in sends(slot, layer, peer_ids):
            copy.start()

    near, far = (4, 8) if grid_x >= 32 else (2, 3)
    offset = jnp.where(me_y == 0, near, far)
    first, last = 0, grid_x - 1
    low_relay, high_relay = first + offset, last - offset
    is_first, is_last = me_x == first, me_x == last
    is_low, is_high = me_x == low_relay, me_x == high_relay
    up_rows, down_rows = 3 * width // 2, width
    top = layers - 1

    def at_x(index):
        return {"tx": index}

    def direct_part(peer_idx, start):
        part = pl.ds(start, 2 * width - start)
        return pltpu.make_async_remote_copy(
            src_ref=copies.at[0, top, part],
            dst_ref=recv.at[peer_idx, 0, top, part],
            send_sem=send_sem.at[peer_idx, 0, top],
            recv_sem=recv_sem.at[peer_idx, 0, top],
            device_id=peers[peer_idx],
            device_id_type=MESH,
        )

    def to_relay(peer_idx, size, index):
        return pltpu.make_async_remote_copy(
            src_ref=copies.at[0, top, pl.ds(0, size)],
            dst_ref=relay.at[pl.ds(0, size)],
            send_sem=send_sem.at[peer_idx, 0, top],
            recv_sem=relay_sem.at[0],
            device_id=at_x(index),
            device_id_type=MESH,
        )

    def from_relay(peer_idx, size, index):
        return pltpu.make_async_remote_copy(
            src_ref=relay.at[pl.ds(0, size)],
            dst_ref=recv.at[peer_idx, 0, top, pl.ds(0, size)],
            send_sem=relay_sem.at[1],
            recv_sem=recv_sem.at[peer_idx, 0, top],
            device_id=at_x(index),
            device_id_type=MESH,
        )

    def cast_layer(layer):
        for copy in load_copies(layer):
            copy.wait()
        copies[0, layer, :width, :] = master_one[layer].astype(BF16)
        turned = stage[layer].T
        master_two[layer] = turned
        copies[0, layer, width:, :] = turned.astype(BF16)

    def first_sends(layer):
        start_sends(0, layer, (0, 2))

        @pl.when(jnp.logical_not(is_first))
        def _():
            start_sends(0, layer, (1,))

    for copy in load_copies(top):
        copy.start()

    barrier = pltpu.get_barrier_semaphore()

    def announce(peer):
        pl.semaphore_signal(barrier, inc=1, device_id=peer, device_id_type=MESH)

    announce(peers[1])
    announce(peers[2])

    @pl.when(jnp.logical_not(is_last))
    def _():
        announce(peers[0])

    @pl.when(is_first)
    def _():
        announce(at_x(high_relay))

    @pl.when(is_low)
    def _():
        announce(at_x(first))
        announce(at_x(last))

    @pl.when(is_high)
    def _():
        announce(at_x(last))

    cast_layer(top)
    pl.semaphore_wait(barrier, 3 + 2 * is_last.astype(jnp.int32) + is_high.astype(jnp.int32))

    @pl.when(is_last)
    def _():
        to_relay(0, up_rows, high_relay).start()
        direct_part(0, up_rows).start()
        start_sends(0, top, (1, 2))

    @pl.when(is_first)
    def _():
        to_relay(1, down_rows, low_relay).start()

    @pl.when(jnp.logical_not(is_last))
    def _():
        first_sends(top)

    for layer in reversed(range(top)):
        for copy in load_copies(layer):
            copy.start()
    acts_copy(0).start()
    goals_copy(0).start()

    @pl.when(is_last)
    def _():
        for index in (first, low_relay):
            pl.semaphore_signal(entry_sem, inc=1, device_id=at_x(index), device_id_type=MESH)

    def first_body(idx, carry):
        layer = top - idx
        cast_layer(layer)

        @pl.when(jnp.logical_and(idx == layers // 2, is_high))
        def _():
            to_relay(0, up_rows, high_relay).wait_recv()
            from_relay(0, up_rows, first).start()

        @pl.when(jnp.logical_and(idx == layers // 2, is_low))
        def _():
            to_relay(1, down_rows, low_relay).wait_recv()
            pl.semaphore_wait(entry_sem, 1)
            from_relay(1, down_rows, last).start()

        first_sends(layer)
        return carry

    lax.fori_loop(1, layers, first_body, 0)

    @pl.when(is_first)
    def _():
        pl.semaphore_wait(entry_sem, 1)
        direct_part(1, down_rows).start()

        def late_body(idx, carry):
            start_sends(0, top - idx, (1,))
            return carry

        lax.fori_loop(1, layers, late_body, 0)

    losses[...] = jnp.zeros(losses.shape, F32)

    def step_body(step, carry):
        slot = lax.rem(step, 2)
        later = 1 - slot
        acts_copy(step).wait()

        def forward_body(layer, inner):
            cast_one = copies[slot, layer, :width, :]
            cast_two = copies[slot, layer, width:, :]
            for rows_ds in blocks:
                hid_f = hidden[layer, rows_ds, :].astype(F32)
                inv = lax.rsqrt(jnp.mean(hid_f * hid_f, axis=-1, keepdims=True) + NORM_EPS)
                inv = jnp.broadcast_to(inv, hid_f.shape)
                normed_b = (hid_f * inv).astype(BF16)
                inv_rms[layer, rows_ds, :] = inv
                normed[layer, rows_ds, :] = normed_b
                pre = dot(normed_b, cast_one, 1, 0)
                square = pre * pre
                tanh_v = jnp.tanh(pre * (GELU_SCALE + (GELU_SCALE * GELU_CUBIC) * square))
                cdf = 0.5 + 0.5 * tanh_v
                act_b = (pre * cdf).astype(BF16)
                act[layer, rows_ds, :] = act_b
                inner_slope = 0.5 * GELU_SCALE + (1.5 * GELU_SCALE * GELU_CUBIC) * square
                slope[layer, rows_ds, :] = cdf + (pre * inner_slope) * (1.0 - tanh_v * tanh_v)
                mlp_out = dot(act_b, cast_two, 1, 1)
                hidden[layer + 1, rows_ds, :] = (hid_f + mlp_out).astype(BF16)
            return inner

        lax.fori_loop(0, layers, forward_body, 0)

        @pl.when(step + 1 < steps)
        def _():
            acts_copy(step + 1).start()

        goals_copy(step).wait()
        total = jnp.zeros((8, width), F32)
        for rows_ds in blocks:
            error_term = hidden[layers, rows_ds, :].astype(F32) - goals[rows_ds, :].astype(F32)
            d_hid[rows_ds, :] = (error_term * (2.0 / (rows * width))).astype(BF16)
            total = total + jnp.sum((error_term * error_term).reshape(block // 8, 8, width), axis=0)
        step_loss = jnp.sum(total) / (rows * width)
        lane = lax.broadcasted_iota(jnp.int32, losses.shape, 1)
        losses[...] = jnp.where(lane == step, step_loss, losses[...])

        @pl.when(step + 1 < steps)
        def _():
            goals_copy(step + 1).start()

        def backward_body(idx, inner):
            layer = layers - 1 - idx
            cast_two = copies[slot, layer, width:, :]
            for rows_ds in blocks:
                d_act = dot(d_hid[rows_ds, :], cast_two, 1, 0).astype(BF16).astype(F32)
                d_pre[rows_ds, :] = (d_act * slope[layer, rows_ds, :]).astype(BF16)
            grad_two = dot(d_hid[...], act[layer], 0, 0).astype(BF16)
            grad_one = dot(normed[layer], d_pre[...], 0, 0).astype(BF16)

            for copy in sends(slot, layer):
                copy.wait_recv()

            @pl.when(step > 0)
            def _():
                for copy in sends(later, layer):
                    copy.wait_send()

            for start, grad, master in ((0, grad_one, master_one), (width, grad_two, master_two)):
                part = pl.ds(start, width)
                other = recv[2, slot, layer, part, :].astype(F32)
                mixed = master[layer] + recv[0, slot, layer, part, :].astype(F32)
                mixed = mixed + recv[1, slot, layer, part, :].astype(F32)
                mixed = mixed + other
                mixed = mixed + other
                fresh = mixed * 0.2 - learn_rate * grad.astype(F32)
                master[layer] = fresh
                copies[later, layer, part, :] = fresh.astype(BF16)

            @pl.when(layer > 0)
            def _():
                cast_one = copies[slot, layer, :width, :]
                for rows_ds in blocks:
                    d_normed = dot(d_pre[rows_ds, :], cast_one, 1, 1).astype(BF16).astype(F32)
                    inv = inv_rms[layer, rows_ds, :]
                    normed_f = hidden[layer, rows_ds, :].astype(F32) * inv
                    along = jnp.mean(d_normed * normed_f, axis=-1, keepdims=True)
                    d_in = inv * (d_normed - normed_f * along)
                    d_hid[rows_ds, :] = (d_hid[rows_ds, :].astype(F32) + d_in).astype(BF16)

            @pl.when(step + 1 < steps)
            def _():
                start_sends(later, layer)

            @pl.when(step + 1 == steps)
            def _():
                stage[layer] = master_two[layer].T

            return inner

        lax.fori_loop(0, layers, backward_body, 0)
        return carry

    lax.fori_loop(0, steps, step_body, 0)

    def last_body(layer, carry):
        for copy in sends((steps - 1) % 2, layer):
            copy.wait_send()
        return carry

    lax.fori_loop(0, layers, last_body, 0)

    @pl.when(is_high)
    def _():
        from_relay(0, up_rows, first).wait_send()

    @pl.when(is_low)
    def _():
        from_relay(1, down_rows, last).wait_send()


def write_kernel(one, two, losses, out_one, out_two, out_losses, sems):
    copies = [
        pltpu.make_async_copy(src, dst, sems.at[idx])
        for idx, (src, dst) in enumerate(((one, out_one), (two, out_two), (losses, out_losses)))
    ]
    for copy in copies:
        copy.start()
    for copy in copies:
        copy.wait()


def solution(mesh):
    grid_x = mesh.shape["tx"]

    def device_train(w_one, w_two, inputs, targets):
        layers, width, ffn = w_one.shape[2:]
        steps, rows = inputs.shape[2:4]
        block = min(256, rows)
        dims = (grid_x, steps, layers, rows, width, ffn, block)
        any_spec = pl.BlockSpec(memory_space=pl.ANY)
        vmem_spec = pl.BlockSpec(memory_space=pltpu.VMEM)
        shapes = ((layers, width, ffn), (layers, ffn, width), (1, steps))
        one, two, losses = pl.pallas_call(
            functools.partial(train_kernel, dims),
            out_shape=tuple(pltpu.VMEM(shape, F32) for shape in shapes),
            in_specs=[any_spec] * 4,
            out_specs=(vmem_spec,) * 3,
            scratch_shapes=[
                pltpu.VMEM((layers, width, ffn), F32),
                pltpu.VMEM((2, layers, 2 * width, ffn), BF16),
                pltpu.VMEM((3, 2, layers, 2 * width, ffn), BF16),
                pltpu.VMEM((layers + 1, rows, width), BF16),
                pltpu.VMEM((layers, rows, width), BF16),
                pltpu.VMEM((layers, rows, width), F32),
                pltpu.VMEM((layers, rows, ffn), BF16),
                pltpu.VMEM((layers, rows, ffn), F32),
                pltpu.VMEM((rows, width), BF16),
                pltpu.VMEM((rows, ffn), BF16),
                pltpu.VMEM((rows, width), BF16),
                pltpu.VMEM((2 * width, ffn), BF16),
                pltpu.SemaphoreType.DMA((2, layers)),
                pltpu.SemaphoreType.DMA((2,)),
                pltpu.SemaphoreType.DMA((3, 2, layers)),
                pltpu.SemaphoreType.DMA((3, 2, layers)),
                pltpu.SemaphoreType.DMA((2,)),
                pltpu.SemaphoreType.REGULAR,
            ],
            compiler_params=pltpu.CompilerParams(
                collective_id=0, has_side_effects=True, vmem_limit_bytes=52 * 1024 * 1024
            ),
            name="gossip_train",
        )(w_one[0, 0], w_two[0, 0], inputs[0, 0], targets[0, 0])
        out_one, out_two, out_losses = pl.pallas_call(
            write_kernel,
            out_shape=tuple(jax.ShapeDtypeStruct(shape, F32) for shape in shapes),
            in_specs=[vmem_spec] * 3,
            out_specs=(any_spec,) * 3,
            scratch_shapes=[pltpu.SemaphoreType.DMA((3,))],
            compiler_params=pltpu.CompilerParams(vmem_limit_bytes=1024 * 1024),
            name="write_out",
        )(one, two, losses)
        return out_one[None, None], out_two[None, None], out_losses[None]

    grid_spec = P("tx", "ty")
    return jax.shard_map(
        device_train,
        mesh=mesh,
        in_specs=(grid_spec, grid_spec, grid_spec, grid_spec),
        out_specs=(grid_spec, grid_spec, grid_spec),
        check_vma=False,
    )
```

```python
import functools

import jax
import jax.numpy as jnp
from jax import lax
from jax.experimental import pallas as pl
from jax.experimental.pallas import tpu as pltpu
from jax.sharding import PartitionSpec as P

NORM_EPS = 1e-6
GELU_SCALE = 0.7978845608028654
GELU_CUBIC = 0.044715
MESH = pl.DeviceIdType.MESH
BF16 = jnp.bfloat16
F32 = jnp.float32


def dot(lhs, rhs, lhs_dim, rhs_dim):
    return lax.dot_general(lhs, rhs, (((lhs_dim,), (rhs_dim,)), ((), ())), preferred_element_type=F32)


def train_kernel(
    dims,
    w_one, w_two, inputs, targets,
    master_one, stage, losses,
    master_two, copies, recv, hidden, normed, inv_rms, act, slope, d_hid, d_pre, goals, relay,
    load_sem, data_sem, send_sem, recv_sem, relay_sem, entry_sem,
):
    grid_x, steps, layers, rows, width, ffn, block = dims
    learn_rate = width / (ffn * layers)
    blocks = [pl.ds(start, block) for start in range(0, rows, block)]
    me_x = lax.axis_index("tx")
    me_y = lax.axis_index("ty")
    next_x = lax.rem(me_x + 1, grid_x)
    prev_x = lax.rem(me_x + grid_x - 1, grid_x)
    peers = ({"tx": next_x}, {"tx": prev_x}, {"ty": 1 - me_y})

    def load_copies(layer):
        return (
            pltpu.make_async_copy(w_one.at[layer], master_one.at[layer], load_sem.at[0, layer]),
            pltpu.make_async_copy(w_two.at[layer], stage.at[layer], load_sem.at[1, layer]),
        )

    def acts_copy(step):
        return pltpu.make_async_copy(inputs.at[step], hidden.at[0], data_sem.at[0])

    def goals_copy(step):
        return pltpu.make_async_copy(targets.at[step], goals, data_sem.at[1])

    def sends(slot, layer, peer_ids=(0, 1, 2)):
        return [
            pltpu.make_async_remote_copy(
                src_ref=copies.at[slot, layer],
                dst_ref=recv.at[peer_idx, slot, layer],
                send_sem=send_sem.at[peer_idx, slot, layer],
                recv_sem=recv_sem.at[peer_idx, slot, layer],
                device_id=peers[peer_idx],
                device_id_type=MESH,
            )
            for peer_idx in peer_ids
        ]

    def start_sends(slot, layer, peer_ids=(0, 1, 2)):
        for copy in sends(slot, layer, peer_ids):
            copy.start()

    first, last = 0, grid_x - 1
    up_relay, down_relay = first + 3, last - 3
    is_first, is_last = me_x == first, me_x == last
    is_up, is_down = me_x == up_relay, me_x == down_relay
    up_rows, down_rows = 9 * width // 8, 5 * width // 8
    top = layers - 1

    def at_x(index):
        return {"tx": index}

    def direct_part(peer_idx, start):
        part = pl.ds(start, 2 * width - start)
        return pltpu.make_async_remote_copy(
            src_ref=copies.at[0, top, part],
            dst_ref=recv.at[peer_idx, 0, top, part],
            send_sem=send_sem.at[peer_idx, 0, top],
            recv_sem=recv_sem.at[peer_idx, 0, top],
            device_id=peers[peer_idx],
            device_id_type=MESH,
        )

    def to_relay(peer_idx, size, index):
        return pltpu.make_async_remote_copy(
            src_ref=copies.at[0, top, pl.ds(0, size)],
            dst_ref=relay.at[pl.ds(0, size)],
            send_sem=send_sem.at[peer_idx, 0, top],
            recv_sem=relay_sem.at[0],
            device_id=at_x(index),
            device_id_type=MESH,
        )

    def from_relay(peer_idx, size, index):
        return pltpu.make_async_remote_copy(
            src_ref=relay.at[pl.ds(0, size)],
            dst_ref=recv.at[peer_idx, 0, top, pl.ds(0, size)],
            send_sem=relay_sem.at[1],
            recv_sem=recv_sem.at[peer_idx, 0, top],
            device_id=at_x(index),
            device_id_type=MESH,
        )

    def cast_layer(layer):
        for copy in load_copies(layer):
            copy.wait()
        copies[0, layer, :width, :] = master_one[layer].astype(BF16)
        turned = stage[layer].T
        master_two[layer] = turned
        copies[0, layer, width:, :] = turned.astype(BF16)

    def first_sends(layer):
        start_sends(0, layer, (0, 2))

        @pl.when(jnp.logical_not(is_first))
        def _():
            start_sends(0, layer, (1,))

    for copy in load_copies(top):
        copy.start()

    barrier = pltpu.get_barrier_semaphore()

    def announce(peer):
        pl.semaphore_signal(barrier, inc=1, device_id=peer, device_id_type=MESH)

    announce(peers[1])
    announce(peers[2])

    @pl.when(jnp.logical_not(is_last))
    def _():
        announce(peers[0])

    @pl.when(is_first)
    def _():
        announce(at_x(up_relay))

    @pl.when(jnp.logical_or(is_up, is_down))
    def _():
        announce(at_x(last))

    cast_layer(top)
    extra = 2 * is_last.astype(jnp.int32) + is_up.astype(jnp.int32) - is_first.astype(jnp.int32)
    pl.semaphore_wait(barrier, 3 + extra)

    @pl.when(is_last)
    def _():
        to_relay(0, up_rows, up_relay).start()
        direct_part(0, up_rows).start()
        start_sends(0, top, (1, 2))

    @pl.when(jnp.logical_not(is_last))
    def _():
        first_sends(top)

    for layer in reversed(range(top)):
        for copy in load_copies(layer):
            copy.start()
    acts_copy(0).start()
    goals_copy(0).start()

    @pl.when(is_last)
    def _():
        pl.semaphore_signal(entry_sem, inc=1, device_id=peers[0], device_id_type=MESH)

    def first_body(idx, carry):
        layer = top - idx
        cast_layer(layer)

        @pl.when(jnp.logical_and(idx == layers // 2, is_up))
        def _():
            to_relay(0, up_rows, up_relay).wait_recv()
            from_relay(0, up_rows, first).start()

        @pl.when(jnp.logical_and(idx == layers // 2, is_down))
        def _():
            to_relay(1, down_rows, down_relay).wait_recv()
            from_relay(1, down_rows, last).start()

        first_sends(layer)
        return carry

    lax.fori_loop(1, layers, first_body, 0)

    @pl.when(is_first)
    def _():
        pl.semaphore_wait(entry_sem, 1)
        to_relay(1, down_rows, down_relay).start()
        direct_part(1, down_rows).start()

        def late_body(idx, carry):
            start_sends(0, top - idx, (1,))
            return carry

        lax.fori_loop(1, layers, late_body, 0)

    losses[...] = jnp.zeros(losses.shape, F32)

    def step_body(step, carry):
        slot = lax.rem(step, 2)
        later = 1 - slot
        acts_copy(step).wait()

        def forward_body(layer, inner):
            cast_one = copies[slot, layer, :width, :]
            cast_two = copies[slot, layer, width:, :]
            for rows_ds in blocks:
                hid_f = hidden[layer, rows_ds, :].astype(F32)
                inv = lax.rsqrt(jnp.mean(hid_f * hid_f, axis=-1, keepdims=True) + NORM_EPS)
                inv = jnp.broadcast_to(inv, hid_f.shape)
                normed_b = (hid_f * inv).astype(BF16)
                inv_rms[layer, rows_ds, :] = inv
                normed[layer, rows_ds, :] = normed_b
                pre = dot(normed_b, cast_one, 1, 0)
                square = pre * pre
                tanh_v = jnp.tanh(pre * (GELU_SCALE + (GELU_SCALE * GELU_CUBIC) * square))
                cdf = 0.5 + 0.5 * tanh_v
                act_b = (pre * cdf).astype(BF16)
                act[layer, rows_ds, :] = act_b
                inner_slope = 0.5 * GELU_SCALE + (1.5 * GELU_SCALE * GELU_CUBIC) * square
                slope[layer, rows_ds, :] = cdf + (pre * inner_slope) * (1.0 - tanh_v * tanh_v)
                mlp_out = dot(act_b, cast_two, 1, 1)
                hidden[layer + 1, rows_ds, :] = (hid_f + mlp_out).astype(BF16)
            return inner

        lax.fori_loop(0, layers, forward_body, 0)

        @pl.when(step + 1 < steps)
        def _():
            acts_copy(step + 1).start()

        goals_copy(step).wait()
        total = jnp.zeros((8, width), F32)
        for rows_ds in blocks:
            error_term = hidden[layers, rows_ds, :].astype(F32) - goals[rows_ds, :].astype(F32)
            d_hid[rows_ds, :] = (error_term * (2.0 / (rows * width))).astype(BF16)
            total = total + jnp.sum((error_term * error_term).reshape(block // 8, 8, width), axis=0)
        step_loss = jnp.sum(total) / (rows * width)
        lane = lax.broadcasted_iota(jnp.int32, losses.shape, 1)
        losses[...] = jnp.where(lane == step, step_loss, losses[...])

        @pl.when(step + 1 < steps)
        def _():
            goals_copy(step + 1).start()

        def backward_body(idx, inner):
            layer = layers - 1 - idx
            cast_two = copies[slot, layer, width:, :]
            for rows_ds in blocks:
                d_act = dot(d_hid[rows_ds, :], cast_two, 1, 0).astype(BF16).astype(F32)
                d_pre[rows_ds, :] = (d_act * slope[layer, rows_ds, :]).astype(BF16)
            grad_two = dot(d_hid[...], act[layer], 0, 0).astype(BF16)
            grad_one = dot(normed[layer], d_pre[...], 0, 0).astype(BF16)

            for copy in sends(slot, layer):
                copy.wait_recv()

            @pl.when(step > 0)
            def _():
                for copy in sends(later, layer):
                    copy.wait_send()

            for start, grad, master in ((0, grad_one, master_one), (width, grad_two, master_two)):
                part = pl.ds(start, width)
                other = recv[2, slot, layer, part, :].astype(F32)
                mixed = master[layer] + recv[0, slot, layer, part, :].astype(F32)
                mixed = mixed + recv[1, slot, layer, part, :].astype(F32)
                mixed = mixed + other
                mixed = mixed + other
                fresh = mixed * 0.2 - learn_rate * grad.astype(F32)
                master[layer] = fresh
                copies[later, layer, part, :] = fresh.astype(BF16)

            @pl.when(layer > 0)
            def _():
                cast_one = copies[slot, layer, :width, :]
                for rows_ds in blocks:
                    d_normed = dot(d_pre[rows_ds, :], cast_one, 1, 1).astype(BF16).astype(F32)
                    inv = inv_rms[layer, rows_ds, :]
                    normed_f = hidden[layer, rows_ds, :].astype(F32) * inv
                    along = jnp.mean(d_normed * normed_f, axis=-1, keepdims=True)
                    d_in = inv * (d_normed - normed_f * along)
                    d_hid[rows_ds, :] = (d_hid[rows_ds, :].astype(F32) + d_in).astype(BF16)

            @pl.when(step + 1 < steps)
            def _():
                start_sends(later, layer)

            @pl.when(step + 1 == steps)
            def _():
                stage[layer] = master_two[layer].T

            return inner

        lax.fori_loop(0, layers, backward_body, 0)
        return carry

    lax.fori_loop(0, steps, step_body, 0)

    def last_body(layer, carry):
        for copy in sends((steps - 1) % 2, layer):
            copy.wait_send()
        return carry

    lax.fori_loop(0, layers, last_body, 0)

    @pl.when(is_up)
    def _():
        from_relay(0, up_rows, first).wait_send()

    @pl.when(is_down)
    def _():
        from_relay(1, down_rows, last).wait_send()


def write_kernel(one, two, losses, out_one, out_two, out_losses, sems):
    copies = [
        pltpu.make_async_copy(src, dst, sems.at[idx])
        for idx, (src, dst) in enumerate(((one, out_one), (two, out_two), (losses, out_losses)))
    ]
    for copy in copies:
        copy.start()
    for copy in copies:
        copy.wait()


def solution(mesh):
    grid_x = mesh.shape["tx"]

    def device_train(w_one, w_two, inputs, targets):
        layers, width, ffn = w_one.shape[2:]
        steps, rows = inputs.shape[2:4]
        block = min(256, rows)
        dims = (grid_x, steps, layers, rows, width, ffn, block)
        any_spec = pl.BlockSpec(memory_space=pl.ANY)
        vmem_spec = pl.BlockSpec(memory_space=pltpu.VMEM)
        shapes = ((layers, width, ffn), (layers, ffn, width), (1, steps))
        one, two, losses = pl.pallas_call(
            functools.partial(train_kernel, dims),
            out_shape=tuple(pltpu.VMEM(shape, F32) for shape in shapes),
            in_specs=[any_spec] * 4,
            out_specs=(vmem_spec,) * 3,
            scratch_shapes=[
                pltpu.VMEM((layers, width, ffn), F32),
                pltpu.VMEM((2, layers, 2 * width, ffn), BF16),
                pltpu.VMEM((3, 2, layers, 2 * width, ffn), BF16),
                pltpu.VMEM((layers + 1, rows, width), BF16),
                pltpu.VMEM((layers, rows, width), BF16),
                pltpu.VMEM((layers, rows, width), F32),
                pltpu.VMEM((layers, rows, ffn), BF16),
                pltpu.VMEM((layers, rows, ffn), F32),
                pltpu.VMEM((rows, width), BF16),
                pltpu.VMEM((rows, ffn), BF16),
                pltpu.VMEM((rows, width), BF16),
                pltpu.VMEM((2 * width, ffn), BF16),
                pltpu.SemaphoreType.DMA((2, layers)),
                pltpu.SemaphoreType.DMA((2,)),
                pltpu.SemaphoreType.DMA((3, 2, layers)),
                pltpu.SemaphoreType.DMA((3, 2, layers)),
                pltpu.SemaphoreType.DMA((2,)),
                pltpu.SemaphoreType.REGULAR,
            ],
            compiler_params=pltpu.CompilerParams(
                collective_id=0, has_side_effects=True, vmem_limit_bytes=52 * 1024 * 1024
            ),
            name="gossip_train",
        )(w_one[0, 0], w_two[0, 0], inputs[0, 0], targets[0, 0])
        out_one, out_two, out_losses = pl.pallas_call(
            write_kernel,
            out_shape=tuple(jax.ShapeDtypeStruct(shape, F32) for shape in shapes),
            in_specs=[vmem_spec] * 3,
            out_specs=(any_spec,) * 3,
            scratch_shapes=[pltpu.SemaphoreType.DMA((3,))],
            compiler_params=pltpu.CompilerParams(vmem_limit_bytes=1024 * 1024),
            name="write_out",
        )(one, two, losses)
        return out_one[None, None], out_two[None, None], out_losses[None]

    grid_spec = P("tx", "ty")
    return jax.shard_map(
        device_train,
        mesh=mesh,
        in_specs=(grid_spec, grid_spec, grid_spec, grid_spec),
        out_specs=(grid_spec, grid_spec, grid_spec),
        check_vma=False,
    )
```

```python
import functools

import jax
import jax.numpy as jnp
from jax import lax
from jax.experimental import pallas as pl
from jax.experimental.pallas import tpu as pltpu
from jax.sharding import PartitionSpec as P

NORM_EPS = 1e-6
GELU_SCALE = 0.7978845608028654
GELU_CUBIC = 0.044715
MESH = pl.DeviceIdType.MESH
BF16 = jnp.bfloat16
F32 = jnp.float32


def dot(lhs, rhs, lhs_dim, rhs_dim):
    return lax.dot_general(lhs, rhs, (((lhs_dim,), (rhs_dim,)), ((), ())), preferred_element_type=F32)


def train_kernel(
    dims,
    w_one, w_two, inputs, targets,
    master_one, stage, losses,
    master_two, copies, recv, hidden, normed, inv_rms, act, slope, d_hid, d_pre, goals, relay,
    load_sem, data_sem, send_sem, recv_sem, relay_sem, entry_sem,
):
    grid_x, steps, layers, rows, width, ffn, block = dims
    learn_rate = width / (ffn * layers)
    blocks = [pl.ds(start, block) for start in range(0, rows, block)]
    me_x = lax.axis_index("tx")
    me_y = lax.axis_index("ty")
    next_x = lax.rem(me_x + 1, grid_x)
    prev_x = lax.rem(me_x + grid_x - 1, grid_x)
    peers = ({"tx": next_x}, {"tx": prev_x}, {"ty": 1 - me_y})

    def load_copies(layer):
        return (
            pltpu.make_async_copy(w_one.at[layer], master_one.at[layer], load_sem.at[0, layer]),
            pltpu.make_async_copy(w_two.at[layer], stage.at[layer], load_sem.at[1, layer]),
        )

    def acts_copy(step):
        return pltpu.make_async_copy(inputs.at[step], hidden.at[0], data_sem.at[0])

    def goals_copy(step):
        return pltpu.make_async_copy(targets.at[step], goals, data_sem.at[1])

    def sends(slot, layer, peer_ids=(0, 1, 2)):
        return [
            pltpu.make_async_remote_copy(
                src_ref=copies.at[slot, layer],
                dst_ref=recv.at[peer_idx, slot, layer],
                send_sem=send_sem.at[peer_idx, slot, layer],
                recv_sem=recv_sem.at[peer_idx, slot, layer],
                device_id=peers[peer_idx],
                device_id_type=MESH,
            )
            for peer_idx in peer_ids
        ]

    def start_sends(slot, layer, peer_ids=(0, 1, 2)):
        for copy in sends(slot, layer, peer_ids):
            copy.start()

    plane, near, far = (16, 3, 7) if grid_x >= 32 else (8, 2, 3)
    place = lax.rem(me_x, plane)
    ring_first, ring_last = me_x == 0, me_x == grid_x - 1
    is_first, is_last = place == 0, place == plane - 1
    is_up, is_down = place == near, place == plane - 1 - near
    low_end, high_end = me_x < plane, me_x >= grid_x - plane
    is_up_far, is_down_far = me_x == far, me_x == grid_x - 1 - far
    turn_rows, up_rows, down_rows = 3 * width // 8, 3 * width // 4, width // 2
    top = layers - 1

    def both(one, two):
        return jnp.logical_and(one, two)

    def no(flag):
        return jnp.logical_not(flag)

    def shifted(offset):
        return {"tx": lax.rem(me_x + offset + grid_x, grid_x)}

    def direct_part(peer_idx, start):
        part = pl.ds(start, 2 * width - start)
        return pltpu.make_async_remote_copy(
            src_ref=copies.at[0, top, part],
            dst_ref=recv.at[peer_idx, 0, top, part],
            send_sem=send_sem.at[peer_idx, 0, top],
            recv_sem=recv_sem.at[peer_idx, 0, top],
            device_id=peers[peer_idx],
            device_id_type=MESH,
        )

    def to_relay(peer_idx, size):
        return pltpu.make_async_remote_copy(
            src_ref=copies.at[0, top, pl.ds(0, size)],
            dst_ref=relay.at[pl.ds(0, size)],
            send_sem=send_sem.at[peer_idx, 0, top],
            recv_sem=relay_sem.at[0],
            device_id=shifted((1 + near, -1 - near)[peer_idx]),
            device_id_type=MESH,
        )

    def pass_on(peer_idx, size):
        part = pl.ds(size, size)
        return pltpu.make_async_remote_copy(
            src_ref=relay.at[part],
            dst_ref=relay.at[part],
            send_sem=relay_sem.at[2],
            recv_sem=relay_sem.at[0],
            device_id=shifted((far - near, near - far)[peer_idx]),
            device_id_type=MESH,
        )

    def from_relay(peer_idx, start, size, distance):
        part = pl.ds(start, size)
        return pltpu.make_async_remote_copy(
            src_ref=relay.at[part],
            dst_ref=recv.at[peer_idx, 0, top, part],
            send_sem=relay_sem.at[1],
            recv_sem=recv_sem.at[peer_idx, 0, top],
            device_id=shifted((-distance, distance)[peer_idx]),
            device_id_type=MESH,
        )

    relays = (
        (0, is_up, low_end, is_up_far, up_rows),
        (1, is_down, high_end, is_down_far, down_rows),
    )

    def relay_near():
        for peer_idx, is_near, is_end, _, size in relays:

            @pl.when(both(is_near, is_end))
            def _():
                to_relay(peer_idx, 2 * size).wait_recv()
                pass_on(peer_idx, size).start()
                from_relay(peer_idx, 0, size, near).start()

            @pl.when(both(is_near, no(is_end)))
            def _():
                to_relay(peer_idx, turn_rows).wait_recv()
                from_relay(peer_idx, 0, turn_rows, near).start()

    def relay_far():
        for peer_idx, _, _, is_far, size in relays:

            @pl.when(is_far)
            def _():
                pass_on(peer_idx, size).wait_recv()
                from_relay(peer_idx, size, size, far).start()

    def relay_end():
        for peer_idx, is_near, is_end, is_far, size in relays:

            @pl.when(both(is_near, is_end))
            def _():
                pass_on(peer_idx, size).wait_send()
                from_relay(peer_idx, 0, size, near).wait_send()

            @pl.when(both(is_near, no(is_end)))
            def _():
                from_relay(peer_idx, 0, turn_rows, near).wait_send()

            @pl.when(is_far)
            def _():
                from_relay(peer_idx, size, size, far).wait_send()

    def turn_sends(peer_idx, size):
        to_relay(peer_idx, size).start()
        direct_part(peer_idx, size).start()

    def cast_layer(layer):
        for copy in load_copies(layer):
            copy.wait()
        copies[0, layer, :width, :] = master_one[layer].astype(BF16)
        turned = stage[layer].T
        master_two[layer] = turned
        copies[0, layer, width:, :] = turned.astype(BF16)

    def first_sends(layer):
        start_sends(0, layer, (0, 2))

        @pl.when(no(ring_first))
        def _():
            start_sends(0, layer, (1,))

    for copy in load_copies(top):
        copy.start()

    barrier = pltpu.get_barrier_semaphore()

    def announce(peer):
        pl.semaphore_signal(barrier, inc=1, device_id=peer, device_id_type=MESH)

    announce(peers[1])
    announce(peers[2])

    @pl.when(no(ring_last))
    def _():
        announce(peers[0])

    @pl.when(is_first)
    def _():
        announce(shifted(near))

    @pl.when(is_up)
    def _():
        announce(shifted(-1 - near))

    @pl.when(both(is_down, high_end))
    def _():
        announce(shifted(near))

    @pl.when(both(is_down, no(high_end)))
    def _():
        announce(shifted(1 + near))

    @pl.when(is_up_far)
    def _():
        announce(shifted(near - far))

    @pl.when(is_down_far)
    def _():
        announce(shifted(far - near))

    cast_layer(top)
    expected = 3
    for flag in (is_first, is_last, ring_last, is_up, both(is_up, low_end), both(is_down, high_end)):
        expected = expected + flag.astype(jnp.int32)
    pl.semaphore_wait(barrier, expected - 2 * ring_first.astype(jnp.int32))

    start_sends(0, top, (2,))

    @pl.when(ring_last)
    def _():
        turn_sends(0, 2 * up_rows)

    @pl.when(both(is_last, no(ring_last)))
    def _():
        turn_sends(0, turn_rows)

    @pl.when(no(is_last))
    def _():
        start_sends(0, top, (0,))

    @pl.when(both(is_first, no(ring_first)))
    def _():
        turn_sends(1, turn_rows)

    @pl.when(no(is_first))
    def _():
        start_sends(0, top, (1,))

    for layer in reversed(range(top)):
        for copy in load_copies(layer):
            copy.start()
    acts_copy(0).start()
    goals_copy(0).start()

    @pl.when(ring_last)
    def _():
        pl.semaphore_signal(entry_sem, inc=1, device_id=peers[0], device_id_type=MESH)

    def first_body(idx, carry):
        layer = top - idx
        cast_layer(layer)

        @pl.when(idx == layers // 2)
        def _():
            relay_near()

        @pl.when(idx == (layers + 2) // 2)
        def _():
            relay_far()

        first_sends(layer)
        return carry

    lax.fori_loop(1, layers, first_body, 0)

    @pl.when(ring_first)
    def _():
        pl.semaphore_wait(entry_sem, 1)
        turn_sends(1, 2 * down_rows)

        def late_body(idx, carry):
            start_sends(0, top - idx, (1,))
            return carry

        lax.fori_loop(1, layers, late_body, 0)

    losses[...] = jnp.zeros(losses.shape, F32)

    def step_body(step, carry):
        slot = lax.rem(step, 2)
        later = 1 - slot
        acts_copy(step).wait()

        def forward_body(layer, inner):
            cast_one = copies[slot, layer, :width, :]
            cast_two = copies[slot, layer, width:, :]
            for rows_ds in blocks:
                hid_f = hidden[layer, rows_ds, :].astype(F32)
                inv = lax.rsqrt(jnp.mean(hid_f * hid_f, axis=-1, keepdims=True) + NORM_EPS)
                inv = jnp.broadcast_to(inv, hid_f.shape)
                normed_b = (hid_f * inv).astype(BF16)
                inv_rms[layer, rows_ds, :] = inv
                normed[layer, rows_ds, :] = normed_b
                pre = dot(normed_b, cast_one, 1, 0)
                square = pre * pre
                tanh_v = jnp.tanh(pre * (GELU_SCALE + (GELU_SCALE * GELU_CUBIC) * square))
                cdf = 0.5 + 0.5 * tanh_v
                act_b = (pre * cdf).astype(BF16)
                act[layer, rows_ds, :] = act_b
                inner_slope = 0.5 * GELU_SCALE + (1.5 * GELU_SCALE * GELU_CUBIC) * square
                slope[layer, rows_ds, :] = cdf + (pre * inner_slope) * (1.0 - tanh_v * tanh_v)
                mlp_out = dot(act_b, cast_two, 1, 1)
                hidden[layer + 1, rows_ds, :] = (hid_f + mlp_out).astype(BF16)
            return inner

        lax.fori_loop(0, layers, forward_body, 0)

        @pl.when(step + 1 < steps)
        def _():
            acts_copy(step + 1).start()

        goals_copy(step).wait()
        total = jnp.zeros((8, width), F32)
        for rows_ds in blocks:
            error_term = hidden[layers, rows_ds, :].astype(F32) - goals[rows_ds, :].astype(F32)
            d_hid[rows_ds, :] = (error_term * (2.0 / (rows * width))).astype(BF16)
            total = total + jnp.sum((error_term * error_term).reshape(block // 8, 8, width), axis=0)
        step_loss = jnp.sum(total) / (rows * width)
        lane = lax.broadcasted_iota(jnp.int32, losses.shape, 1)
        losses[...] = jnp.where(lane == step, step_loss, losses[...])

        @pl.when(step + 1 < steps)
        def _():
            goals_copy(step + 1).start()

        def backward_body(idx, inner):
            layer = layers - 1 - idx
            cast_two = copies[slot, layer, width:, :]
            for rows_ds in blocks:
                d_act = dot(d_hid[rows_ds, :], cast_two, 1, 0).astype(BF16).astype(F32)
                d_pre[rows_ds, :] = (d_act * slope[layer, rows_ds, :]).astype(BF16)
            grad_two = dot(d_hid[...], act[layer], 0, 0).astype(BF16)
            grad_one = dot(normed[layer], d_pre[...], 0, 0).astype(BF16)

            for copy in sends(slot, layer):
                copy.wait_recv()

            @pl.when(step > 0)
            def _():
                for copy in sends(later, layer):
                    copy.wait_send()

            for start, grad, master in ((0, grad_one, master_one), (width, grad_two, master_two)):
                part = pl.ds(start, width)
                other = recv[2, slot, layer, part, :].astype(F32)
                mixed = master[layer] + recv[0, slot, layer, part, :].astype(F32)
                mixed = mixed + recv[1, slot, layer, part, :].astype(F32)
                mixed = mixed + other
                mixed = mixed + other
                fresh = mixed * 0.2 - learn_rate * grad.astype(F32)
                master[layer] = fresh
                copies[later, layer, part, :] = fresh.astype(BF16)

            @pl.when(layer > 0)
            def _():
                cast_one = copies[slot, layer, :width, :]
                for rows_ds in blocks:
                    d_normed = dot(d_pre[rows_ds, :], cast_one, 1, 1).astype(BF16).astype(F32)
                    inv = inv_rms[layer, rows_ds, :]
                    normed_f = hidden[layer, rows_ds, :].astype(F32) * inv
                    along = jnp.mean(d_normed * normed_f, axis=-1, keepdims=True)
                    d_in = inv * (d_normed - normed_f * along)
                    d_hid[rows_ds, :] = (d_hid[rows_ds, :].astype(F32) + d_in).astype(BF16)

            @pl.when(step + 1 < steps)
            def _():
                start_sends(later, layer)

            @pl.when(step + 1 == steps)
            def _():
                stage[layer] = master_two[layer].T

            return inner

        lax.fori_loop(0, layers, backward_body, 0)
        return carry

    lax.fori_loop(0, steps, step_body, 0)

    def last_body(layer, carry):
        for copy in sends((steps - 1) % 2, layer):
            copy.wait_send()
        return carry

    lax.fori_loop(0, layers, last_body, 0)

    relay_end()


def write_kernel(one, two, losses, out_one, out_two, out_losses, sems):
    copies = [
        pltpu.make_async_copy(src, dst, sems.at[idx])
        for idx, (src, dst) in enumerate(((one, out_one), (two, out_two), (losses, out_losses)))
    ]
    for copy in copies:
        copy.start()
    for copy in copies:
        copy.wait()


def solution(mesh):
    grid_x = mesh.shape["tx"]

    def device_train(w_one, w_two, inputs, targets):
        layers, width, ffn = w_one.shape[2:]
        steps, rows = inputs.shape[2:4]
        block = min(256, rows)
        dims = (grid_x, steps, layers, rows, width, ffn, block)
        any_spec = pl.BlockSpec(memory_space=pl.ANY)
        vmem_spec = pl.BlockSpec(memory_space=pltpu.VMEM)
        shapes = ((layers, width, ffn), (layers, ffn, width), (1, steps))
        one, two, losses = pl.pallas_call(
            functools.partial(train_kernel, dims),
            out_shape=tuple(pltpu.VMEM(shape, F32) for shape in shapes),
            in_specs=[any_spec] * 4,
            out_specs=(vmem_spec,) * 3,
            scratch_shapes=[
                pltpu.VMEM((layers, width, ffn), F32),
                pltpu.VMEM((2, layers, 2 * width, ffn), BF16),
                pltpu.VMEM((3, 2, layers, 2 * width, ffn), BF16),
                pltpu.VMEM((layers + 1, rows, width), BF16),
                pltpu.VMEM((layers, rows, width), BF16),
                pltpu.VMEM((layers, rows, width), F32),
                pltpu.VMEM((layers, rows, ffn), BF16),
                pltpu.VMEM((layers, rows, ffn), F32),
                pltpu.VMEM((rows, width), BF16),
                pltpu.VMEM((rows, ffn), BF16),
                pltpu.VMEM((rows, width), BF16),
                pltpu.VMEM((2 * width, ffn), BF16),
                pltpu.SemaphoreType.DMA((2, layers)),
                pltpu.SemaphoreType.DMA((2,)),
                pltpu.SemaphoreType.DMA((3, 2, layers)),
                pltpu.SemaphoreType.DMA((3, 2, layers)),
                pltpu.SemaphoreType.DMA((3,)),
                pltpu.SemaphoreType.REGULAR,
            ],
            compiler_params=pltpu.CompilerParams(
                collective_id=0, has_side_effects=True, vmem_limit_bytes=52 * 1024 * 1024
            ),
            name="gossip_train",
        )(w_one[0, 0], w_two[0, 0], inputs[0, 0], targets[0, 0])
        out_one, out_two, out_losses = pl.pallas_call(
            write_kernel,
            out_shape=tuple(jax.ShapeDtypeStruct(shape, F32) for shape in shapes),
            in_specs=[vmem_spec] * 3,
            out_specs=(any_spec,) * 3,
            scratch_shapes=[pltpu.SemaphoreType.DMA((3,))],
            compiler_params=pltpu.CompilerParams(vmem_limit_bytes=1024 * 1024),
            name="write_out",
        )(one, two, losses)
        return out_one[None, None], out_two[None, None], out_losses[None]

    grid_spec = P("tx", "ty")
    return jax.shard_map(
        device_train,
        mesh=mesh,
        in_specs=(grid_spec, grid_spec, grid_spec, grid_spec),
        out_specs=(grid_spec, grid_spec, grid_spec),
        check_vma=False,
    )
```

```python
import functools

import jax
import jax.numpy as jnp
from jax import lax
from jax.experimental import pallas as pl
from jax.experimental.pallas import tpu as pltpu
from jax.sharding import PartitionSpec as P

NORM_EPS = 1e-6
GELU_SCALE = 0.7978845608028654
GELU_CUBIC = 0.044715
MESH = pl.DeviceIdType.MESH
BF16 = jnp.bfloat16
F32 = jnp.float32


def dot(lhs, rhs, lhs_dim, rhs_dim):
    return lax.dot_general(lhs, rhs, (((lhs_dim,), (rhs_dim,)), ((), ())), preferred_element_type=F32)


def train_kernel(
    dims,
    w_one, w_two, inputs, targets,
    master_one, stage, losses,
    master_two, copies, recv, hidden, normed, inv_rms, act, slope, d_hid, d_pre, goals, relay,
    load_sem, data_sem, send_sem, recv_sem, relay_sem, tail_sem, entry_sem,
):
    grid_x, steps, layers, rows, width, ffn, block = dims
    learn_rate = width / (ffn * layers)
    blocks = [pl.ds(start, block) for start in range(0, rows, block)]
    me_x = lax.axis_index("tx")
    me_y = lax.axis_index("ty")
    next_x = lax.rem(me_x + 1, grid_x)
    prev_x = lax.rem(me_x + grid_x - 1, grid_x)
    peers = ({"tx": next_x}, {"tx": prev_x}, {"ty": 1 - me_y})

    def load_copies(layer):
        return (
            pltpu.make_async_copy(w_one.at[layer], master_one.at[layer], load_sem.at[0, layer]),
            pltpu.make_async_copy(w_two.at[layer], stage.at[layer], load_sem.at[1, layer]),
        )

    def acts_copy(step):
        return pltpu.make_async_copy(inputs.at[step], hidden.at[0], data_sem.at[0])

    def goals_copy(step):
        return pltpu.make_async_copy(targets.at[step], goals, data_sem.at[1])

    def sends(slot, layer, peer_ids=(0, 1, 2)):
        return [
            pltpu.make_async_remote_copy(
                src_ref=copies.at[slot, layer],
                dst_ref=recv.at[peer_idx, slot, layer],
                send_sem=send_sem.at[peer_idx, slot, layer],
                recv_sem=recv_sem.at[peer_idx, slot, layer],
                device_id=peers[peer_idx],
                device_id_type=MESH,
            )
            for peer_idx in peer_ids
        ]

    def tail_half(part):
        slot = (steps - 1) % 2
        half = pl.ds(part * width, width)
        return [
            pltpu.make_async_remote_copy(
                src_ref=copies.at[slot, 0, half],
                dst_ref=recv.at[peer_idx, slot, 0, half],
                send_sem=tail_sem.at[0, peer_idx, part],
                recv_sem=tail_sem.at[1, peer_idx, part],
                device_id=peer,
                device_id_type=MESH,
            )
            for peer_idx, peer in enumerate(peers)
        ]

    def start_sends(slot, layer, peer_ids=(0, 1, 2)):
        for copy in sends(slot, layer, peer_ids):
            copy.start()

    plane, near, far = (16, 3, 7) if grid_x >= 32 else (8, 2, 3)
    place = lax.rem(me_x, plane)
    ring_first, ring_last = me_x == 0, me_x == grid_x - 1
    is_first, is_last = place == 0, place == plane - 1
    is_up, is_down = place == near, place == plane - 1 - near
    low_end, high_end = me_x < plane, me_x >= grid_x - plane
    is_up_far, is_down_far = me_x == far, me_x == grid_x - 1 - far
    turn_rows, up_rows, down_rows = 3 * width // 8, 3 * width // 4, width // 2
    top = layers - 1

    def both(one, two):
        return jnp.logical_and(one, two)

    def no(flag):
        return jnp.logical_not(flag)

    def shifted(offset):
        return {"tx": lax.rem(me_x + offset + grid_x, grid_x)}

    def direct_part(peer_idx, start):
        part = pl.ds(start, 2 * width - start)
        return pltpu.make_async_remote_copy(
            src_ref=copies.at[0, top, part],
            dst_ref=recv.at[peer_idx, 0, top, part],
            send_sem=send_sem.at[peer_idx, 0, top],
            recv_sem=recv_sem.at[peer_idx, 0, top],
            device_id=peers[peer_idx],
            device_id_type=MESH,
        )

    def to_relay(peer_idx, size):
        return pltpu.make_async_remote_copy(
            src_ref=copies.at[0, top, pl.ds(0, size)],
            dst_ref=relay.at[pl.ds(0, size)],
            send_sem=send_sem.at[peer_idx, 0, top],
            recv_sem=relay_sem.at[0],
            device_id=shifted((1 + near, -1 - near)[peer_idx]),
            device_id_type=MESH,
        )

    def pass_on(peer_idx, size):
        part = pl.ds(size, size)
        return pltpu.make_async_remote_copy(
            src_ref=relay.at[part],
            dst_ref=relay.at[part],
            send_sem=relay_sem.at[2],
            recv_sem=relay_sem.at[0],
            device_id=shifted((far - near, near - far)[peer_idx]),
            device_id_type=MESH,
        )

    def from_relay(peer_idx, start, size, distance):
        part = pl.ds(start, size)
        return pltpu.make_async_remote_copy(
            src_ref=relay.at[part],
            dst_ref=recv.at[peer_idx, 0, top, part],
            send_sem=relay_sem.at[1],
            recv_sem=recv_sem.at[peer_idx, 0, top],
            device_id=shifted((-distance, distance)[peer_idx]),
            device_id_type=MESH,
        )

    relays = (
        (0, is_up, low_end, is_up_far, up_rows),
        (1, is_down, high_end, is_down_far, down_rows),
    )

    def relay_near():
        for peer_idx, is_near, is_end, _, size in relays:

            @pl.when(both(is_near, is_end))
            def _():
                to_relay(peer_idx, 2 * size).wait_recv()
                pass_on(peer_idx, size).start()
                from_relay(peer_idx, 0, size, near).start()

            @pl.when(both(is_near, no(is_end)))
            def _():
                to_relay(peer_idx, turn_rows).wait_recv()
                from_relay(peer_idx, 0, turn_rows, near).start()

    def relay_far():
        for peer_idx, _, _, is_far, size in relays:

            @pl.when(is_far)
            def _():
                pass_on(peer_idx, size).wait_recv()
                from_relay(peer_idx, size, size, far).start()

    def relay_end():
        for peer_idx, is_near, is_end, is_far, size in relays:

            @pl.when(both(is_near, is_end))
            def _():
                pass_on(peer_idx, size).wait_send()
                from_relay(peer_idx, 0, size, near).wait_send()

            @pl.when(both(is_near, no(is_end)))
            def _():
                from_relay(peer_idx, 0, turn_rows, near).wait_send()

            @pl.when(is_far)
            def _():
                from_relay(peer_idx, size, size, far).wait_send()

    def turn_sends(peer_idx, size):
        to_relay(peer_idx, size).start()
        direct_part(peer_idx, size).start()

    def cast_layer(layer):
        for copy in load_copies(layer):
            copy.wait()
        copies[0, layer, :width, :] = master_one[layer].astype(BF16)
        turned = stage[layer].T
        master_two[layer] = turned
        copies[0, layer, width:, :] = turned.astype(BF16)

    def first_sends(layer):
        start_sends(0, layer, (0, 2))

        @pl.when(no(ring_first))
        def _():
            start_sends(0, layer, (1,))

    for copy in load_copies(top):
        copy.start()

    barrier = pltpu.get_barrier_semaphore()

    def announce(peer):
        pl.semaphore_signal(barrier, inc=1, device_id=peer, device_id_type=MESH)

    announce(peers[1])
    announce(peers[2])

    @pl.when(no(ring_last))
    def _():
        announce(peers[0])

    @pl.when(is_first)
    def _():
        announce(shifted(near))

    @pl.when(is_up)
    def _():
        announce(shifted(-1 - near))

    @pl.when(both(is_down, high_end))
    def _():
        announce(shifted(near))

    @pl.when(both(is_down, no(high_end)))
    def _():
        announce(shifted(1 + near))

    @pl.when(is_up_far)
    def _():
        announce(shifted(near - far))

    @pl.when(is_down_far)
    def _():
        announce(shifted(far - near))

    cast_layer(top)
    expected = 3
    for flag in (is_first, is_last, ring_last, is_up, both(is_up, low_end), both(is_down, high_end)):
        expected = expected + flag.astype(jnp.int32)
    pl.semaphore_wait(barrier, expected - 2 * ring_first.astype(jnp.int32))

    start_sends(0, top, (2,))

    @pl.when(ring_last)
    def _():
        turn_sends(0, 2 * up_rows)

    @pl.when(both(is_last, no(ring_last)))
    def _():
        turn_sends(0, turn_rows)

    @pl.when(no(is_last))
    def _():
        start_sends(0, top, (0,))

    @pl.when(both(is_first, no(ring_first)))
    def _():
        turn_sends(1, turn_rows)

    @pl.when(no(is_first))
    def _():
        start_sends(0, top, (1,))

    for layer in reversed(range(top)):
        for copy in load_copies(layer):
            copy.start()
    acts_copy(0).start()
    goals_copy(0).start()

    @pl.when(ring_last)
    def _():
        pl.semaphore_signal(entry_sem, inc=1, device_id=peers[0], device_id_type=MESH)

    def first_body(idx, carry):
        layer = top - idx
        cast_layer(layer)

        @pl.when(idx == layers // 2)
        def _():
            relay_near()

        @pl.when(idx == (layers + 2) // 2)
        def _():
            relay_far()

        first_sends(layer)
        return carry

    lax.fori_loop(1, layers, first_body, 0)

    @pl.when(ring_first)
    def _():
        pl.semaphore_wait(entry_sem, 1)
        turn_sends(1, 2 * down_rows)

        def late_body(idx, carry):
            start_sends(0, top - idx, (1,))
            return carry

        lax.fori_loop(1, layers, late_body, 0)

    losses[...] = jnp.zeros(losses.shape, F32)

    def step_body(step, carry):
        slot = lax.rem(step, 2)
        later = 1 - slot
        acts_copy(step).wait()

        def forward_body(layer, inner):
            cast_one = copies[slot, layer, :width, :]
            cast_two = copies[slot, layer, width:, :]
            for rows_ds in blocks:
                hid_f = hidden[layer, rows_ds, :].astype(F32)
                inv = lax.rsqrt(jnp.mean(hid_f * hid_f, axis=-1, keepdims=True) + NORM_EPS)
                inv = jnp.broadcast_to(inv, hid_f.shape)
                normed_b = (hid_f * inv).astype(BF16)
                inv_rms[layer, rows_ds, :] = inv
                normed[layer, rows_ds, :] = normed_b
                pre = dot(normed_b, cast_one, 1, 0)
                square = pre * pre
                tanh_v = jnp.tanh(pre * (GELU_SCALE + (GELU_SCALE * GELU_CUBIC) * square))
                cdf = 0.5 + 0.5 * tanh_v
                act_b = (pre * cdf).astype(BF16)
                act[layer, rows_ds, :] = act_b
                inner_slope = 0.5 * GELU_SCALE + (1.5 * GELU_SCALE * GELU_CUBIC) * square
                slope[layer, rows_ds, :] = cdf + (pre * inner_slope) * (1.0 - tanh_v * tanh_v)
                mlp_out = dot(act_b, cast_two, 1, 1)
                hidden[layer + 1, rows_ds, :] = (hid_f + mlp_out).astype(BF16)
            return inner

        lax.fori_loop(0, layers, forward_body, 0)

        @pl.when(step + 1 < steps)
        def _():
            acts_copy(step + 1).start()

        goals_copy(step).wait()
        total = jnp.zeros((8, width), F32)
        for rows_ds in blocks:
            error_term = hidden[layers, rows_ds, :].astype(F32) - goals[rows_ds, :].astype(F32)
            d_hid[rows_ds, :] = (error_term * (2.0 / (rows * width))).astype(BF16)
            total = total + jnp.sum((error_term * error_term).reshape(block // 8, 8, width), axis=0)
        step_loss = jnp.sum(total) / (rows * width)
        lane = lax.broadcasted_iota(jnp.int32, losses.shape, 1)
        losses[...] = jnp.where(lane == step, step_loss, losses[...])

        @pl.when(step + 1 < steps)
        def _():
            goals_copy(step + 1).start()

        def backward_body(idx, inner):
            layer = layers - 1 - idx
            cast_two = copies[slot, layer, width:, :]
            for rows_ds in blocks:
                d_act = dot(d_hid[rows_ds, :], cast_two, 1, 0).astype(BF16).astype(F32)
                d_pre[rows_ds, :] = (d_act * slope[layer, rows_ds, :]).astype(BF16)
            grad_two = dot(d_hid[...], act[layer], 0, 0).astype(BF16)
            grad_one = dot(normed[layer], d_pre[...], 0, 0).astype(BF16)

            is_tail = both(step + 1 == steps, layer == 0)

            @pl.when(no(is_tail))
            def _():
                for copy in sends(slot, layer):
                    copy.wait_recv()

            @pl.when(is_tail)
            def _():
                for copy in tail_half(1):
                    copy.wait_recv()

            @pl.when(step > 0)
            def _():
                for copy in sends(later, layer):
                    copy.wait_send()

            def update(start, grad, master):
                part = pl.ds(start, width)
                other = recv[2, slot, layer, part, :].astype(F32)
                mixed = master[layer] + recv[0, slot, layer, part, :].astype(F32)
                mixed = mixed + recv[1, slot, layer, part, :].astype(F32)
                mixed = mixed + other
                mixed = mixed + other
                fresh = mixed * 0.2 - learn_rate * grad.astype(F32)
                master[layer] = fresh
                copies[later, layer, part, :] = fresh.astype(BF16)

            update(width, grad_two, master_two)

            @pl.when(step + 1 == steps)
            def _():
                stage[layer] = master_two[layer].T

            @pl.when(is_tail)
            def _():
                for copy in tail_half(0):
                    copy.wait_recv()

            update(0, grad_one, master_one)

            @pl.when(layer > 0)
            def _():
                cast_one = copies[slot, layer, :width, :]
                for rows_ds in blocks:
                    d_normed = dot(d_pre[rows_ds, :], cast_one, 1, 1).astype(BF16).astype(F32)
                    inv = inv_rms[layer, rows_ds, :]
                    normed_f = hidden[layer, rows_ds, :].astype(F32) * inv
                    along = jnp.mean(d_normed * normed_f, axis=-1, keepdims=True)
                    d_in = inv * (d_normed - normed_f * along)
                    d_hid[rows_ds, :] = (d_hid[rows_ds, :].astype(F32) + d_in).astype(BF16)

            to_tail = both(step + 2 == steps, layer == 0)

            @pl.when(both(step + 1 < steps, no(to_tail)))
            def _():
                start_sends(later, layer)

            @pl.when(to_tail)
            def _():
                for copy in tail_half(1) + tail_half(0):
                    copy.start()

            return inner

        lax.fori_loop(0, layers, backward_body, 0)
        return carry

    lax.fori_loop(0, steps, step_body, 0)

    def last_body(layer, carry):
        for copy in sends((steps - 1) % 2, layer):
            copy.wait_send()
        return carry

    lax.fori_loop(1, layers, last_body, 0)
    for copy in tail_half(1) + tail_half(0):
        copy.wait_send()

    relay_end()


def write_kernel(one, two, losses, out_one, out_two, out_losses, sems):
    pairs = [(losses, out_losses)]
    for layer in range(one.shape[0]):
        pairs += [(one.at[layer], out_one.at[layer]), (two.at[layer], out_two.at[layer])]
    copies = [pltpu.make_async_copy(src, dst, sems.at[idx]) for idx, (src, dst) in enumerate(pairs)]
    for copy in copies:
        copy.start()
    for copy in copies:
        copy.wait()


def solution(mesh):
    grid_x = mesh.shape["tx"]

    def device_train(w_one, w_two, inputs, targets):
        layers, width, ffn = w_one.shape[2:]
        steps, rows = inputs.shape[2:4]
        block = min(256, rows)
        dims = (grid_x, steps, layers, rows, width, ffn, block)
        any_spec = pl.BlockSpec(memory_space=pl.ANY)
        vmem_spec = pl.BlockSpec(memory_space=pltpu.VMEM)
        shapes = ((layers, width, ffn), (layers, ffn, width), (1, steps))
        one, two, losses = pl.pallas_call(
            functools.partial(train_kernel, dims),
            out_shape=tuple(pltpu.VMEM(shape, F32) for shape in shapes),
            in_specs=[any_spec] * 4,
            out_specs=(vmem_spec,) * 3,
            scratch_shapes=[
                pltpu.VMEM((layers, width, ffn), F32),
                pltpu.VMEM((2, layers, 2 * width, ffn), BF16),
                pltpu.VMEM((3, 2, layers, 2 * width, ffn), BF16),
                pltpu.VMEM((layers + 1, rows, width), BF16),
                pltpu.VMEM((layers, rows, width), BF16),
                pltpu.VMEM((layers, rows, width), F32),
                pltpu.VMEM((layers, rows, ffn), BF16),
                pltpu.VMEM((layers, rows, ffn), F32),
                pltpu.VMEM((rows, width), BF16),
                pltpu.VMEM((rows, ffn), BF16),
                pltpu.VMEM((rows, width), BF16),
                pltpu.VMEM((2 * width, ffn), BF16),
                pltpu.SemaphoreType.DMA((2, layers)),
                pltpu.SemaphoreType.DMA((2,)),
                pltpu.SemaphoreType.DMA((3, 2, layers)),
                pltpu.SemaphoreType.DMA((3, 2, layers)),
                pltpu.SemaphoreType.DMA((3,)),
                pltpu.SemaphoreType.DMA((2, 3, 2)),
                pltpu.SemaphoreType.REGULAR,
            ],
            compiler_params=pltpu.CompilerParams(
                collective_id=0, has_side_effects=True, vmem_limit_bytes=52 * 1024 * 1024
            ),
            name="gossip_train",
        )(w_one[0, 0], w_two[0, 0], inputs[0, 0], targets[0, 0])
        out_one, out_two, out_losses = pl.pallas_call(
            write_kernel,
            out_shape=tuple(jax.ShapeDtypeStruct(shape, F32) for shape in shapes),
            in_specs=[vmem_spec] * 3,
            out_specs=(any_spec,) * 3,
            scratch_shapes=[pltpu.SemaphoreType.DMA((2 * layers + 1,))],
            compiler_params=pltpu.CompilerParams(vmem_limit_bytes=1024 * 1024),
            name="write_out",
        )(one, two, losses)
        return out_one[None, None], out_two[None, None], out_losses[None]

    grid_spec = P("tx", "ty")
    return jax.shard_map(
        device_train,
        mesh=mesh,
        in_specs=(grid_spec, grid_spec, grid_spec, grid_spec),
        out_specs=(grid_spec, grid_spec, grid_spec),
        check_vma=False,
    )
```

```python
import functools

import jax
import jax.numpy as jnp
from jax import lax
from jax.experimental import pallas as pl
from jax.experimental.pallas import tpu as pltpu
from jax.sharding import PartitionSpec as P

NORM_EPS = 1e-6
GELU_SCALE = 0.7978845608028654
GELU_CUBIC = 0.044715
MESH = pl.DeviceIdType.MESH
BF16 = jnp.bfloat16
F32 = jnp.float32


def dot(lhs, rhs, lhs_dim, rhs_dim):
    return lax.dot_general(lhs, rhs, (((lhs_dim,), (rhs_dim,)), ((), ())), preferred_element_type=F32)


def train_kernel(
    dims,
    w_one, w_two, inputs, targets,
    master_one, stage, losses,
    master_two, copies, recv, hidden, normed, inv_rms, act, slope, d_hid, d_pre, goals, relay,
    load_sem, data_sem, send_sem, recv_sem, relay_sem, tail_sem, entry_sem,
):
    grid_x, steps, layers, rows, width, ffn, block = dims
    learn_rate = width / (ffn * layers)
    blocks = [pl.ds(start, block) for start in range(0, rows, block)]
    me_x = lax.axis_index("tx")
    me_y = lax.axis_index("ty")
    next_x = lax.rem(me_x + 1, grid_x)
    prev_x = lax.rem(me_x + grid_x - 1, grid_x)
    peers = ({"tx": next_x}, {"tx": prev_x}, {"ty": 1 - me_y})

    def load_copies(layer):
        return (
            pltpu.make_async_copy(w_one.at[layer], master_one.at[layer], load_sem.at[0, layer]),
            pltpu.make_async_copy(w_two.at[layer], stage.at[layer], load_sem.at[1, layer]),
        )

    def acts_copy(step):
        return pltpu.make_async_copy(inputs.at[step], hidden.at[0], data_sem.at[0])

    def goals_copy(step):
        return pltpu.make_async_copy(targets.at[step], goals, data_sem.at[1])

    def sends(slot, layer, peer_ids=(0, 1, 2)):
        return [
            pltpu.make_async_remote_copy(
                src_ref=copies.at[slot, layer],
                dst_ref=recv.at[peer_idx, slot, layer],
                send_sem=send_sem.at[peer_idx, slot, layer],
                recv_sem=recv_sem.at[peer_idx, slot, layer],
                device_id=peers[peer_idx],
                device_id_type=MESH,
            )
            for peer_idx in peer_ids
        ]

    def tail_half(part):
        slot = (steps - 1) % 2
        half = pl.ds(part * width, width)
        return [
            pltpu.make_async_remote_copy(
                src_ref=copies.at[slot, 0, half],
                dst_ref=recv.at[peer_idx, slot, 0, half],
                send_sem=tail_sem.at[0, peer_idx, part],
                recv_sem=tail_sem.at[1, peer_idx, part],
                device_id=peer,
                device_id_type=MESH,
            )
            for peer_idx, peer in enumerate(peers)
        ]

    def start_sends(slot, layer, peer_ids=(0, 1, 2)):
        for copy in sends(slot, layer, peer_ids):
            copy.start()

    plane, near, far = (16, 3, 7) if grid_x >= 32 else (8, 2, 3)
    place = lax.rem(me_x, plane)
    ring_first, ring_last = me_x == 0, me_x == grid_x - 1
    is_first, is_last = place == 0, place == plane - 1
    is_up, is_down = place == near, place == plane - 1 - near
    low_end, high_end = me_x < plane, me_x >= grid_x - plane
    is_up_far, is_down_far = me_x == far, me_x == grid_x - 1 - far
    turn_rows, up_rows, down_rows = 3 * width // 8, 3 * width // 4, width // 2
    top = layers - 1

    def both(one, two):
        return jnp.logical_and(one, two)

    def no(flag):
        return jnp.logical_not(flag)

    def shifted(offset):
        return {"tx": lax.rem(me_x + offset + grid_x, grid_x)}

    def direct_part(peer_idx, start):
        part = pl.ds(start, 2 * width - start)
        return pltpu.make_async_remote_copy(
            src_ref=copies.at[0, top, part],
            dst_ref=recv.at[peer_idx, 0, top, part],
            send_sem=send_sem.at[peer_idx, 0, top],
            recv_sem=recv_sem.at[peer_idx, 0, top],
            device_id=peers[peer_idx],
            device_id_type=MESH,
        )

    def to_relay(peer_idx, size):
        return pltpu.make_async_remote_copy(
            src_ref=copies.at[0, top, pl.ds(0, size)],
            dst_ref=relay.at[pl.ds(0, size)],
            send_sem=send_sem.at[peer_idx, 0, top],
            recv_sem=relay_sem.at[0],
            device_id=shifted((1 + near, -1 - near)[peer_idx]),
            device_id_type=MESH,
        )

    def pass_on(peer_idx, size):
        part = pl.ds(size, size)
        return pltpu.make_async_remote_copy(
            src_ref=relay.at[part],
            dst_ref=relay.at[part],
            send_sem=relay_sem.at[2],
            recv_sem=relay_sem.at[0],
            device_id=shifted((far - near, near - far)[peer_idx]),
            device_id_type=MESH,
        )

    def from_relay(peer_idx, start, size, distance):
        part = pl.ds(start, size)
        return pltpu.make_async_remote_copy(
            src_ref=relay.at[part],
            dst_ref=recv.at[peer_idx, 0, top, part],
            send_sem=relay_sem.at[1],
            recv_sem=recv_sem.at[peer_idx, 0, top],
            device_id=shifted((-distance, distance)[peer_idx]),
            device_id_type=MESH,
        )

    relays = (
        (0, is_up, low_end, is_up_far, up_rows),
        (1, is_down, high_end, is_down_far, down_rows),
    )

    def relay_near():
        for peer_idx, is_near, is_end, _, size in relays:

            @pl.when(both(is_near, is_end))
            def _():
                to_relay(peer_idx, 2 * size).wait_recv()
                pass_on(peer_idx, size).start()
                from_relay(peer_idx, 0, size, near).start()

            @pl.when(both(is_near, no(is_end)))
            def _():
                to_relay(peer_idx, turn_rows).wait_recv()
                from_relay(peer_idx, 0, turn_rows, near).start()

    def relay_far():
        for peer_idx, _, _, is_far, size in relays:

            @pl.when(is_far)
            def _():
                pass_on(peer_idx, size).wait_recv()
                from_relay(peer_idx, size, size, far).start()

    def relay_end():
        for peer_idx, is_near, is_end, is_far, size in relays:

            @pl.when(both(is_near, is_end))
            def _():
                pass_on(peer_idx, size).wait_send()
                from_relay(peer_idx, 0, size, near).wait_send()

            @pl.when(both(is_near, no(is_end)))
            def _():
                from_relay(peer_idx, 0, turn_rows, near).wait_send()

            @pl.when(is_far)
            def _():
                from_relay(peer_idx, size, size, far).wait_send()

    def turn_sends(peer_idx, size):
        to_relay(peer_idx, size).start()
        direct_part(peer_idx, size).start()

    def cast_layer(layer):
        for copy in load_copies(layer):
            copy.wait()
        copies[0, layer, :width, :] = master_one[layer].astype(BF16)
        turned = stage[layer].T
        master_two[layer] = turned
        copies[0, layer, width:, :] = turned.astype(BF16)

    def first_sends(layer):
        start_sends(0, layer, (0, 2))

        @pl.when(no(ring_first))
        def _():
            start_sends(0, layer, (1,))

    for copy in load_copies(top):
        copy.start()

    barrier = pltpu.get_barrier_semaphore()

    def announce(peer):
        pl.semaphore_signal(barrier, inc=1, device_id=peer, device_id_type=MESH)

    announce(peers[1])
    announce(peers[2])

    @pl.when(no(ring_last))
    def _():
        announce(peers[0])

    @pl.when(is_first)
    def _():
        announce(shifted(near))

    @pl.when(is_up)
    def _():
        announce(shifted(-1 - near))

    @pl.when(both(is_down, high_end))
    def _():
        announce(shifted(near))

    @pl.when(both(is_down, no(high_end)))
    def _():
        announce(shifted(1 + near))

    @pl.when(is_up_far)
    def _():
        announce(shifted(near - far))

    @pl.when(is_down_far)
    def _():
        announce(shifted(far - near))

    cast_layer(top)
    expected = 3
    for flag in (is_first, is_last, ring_last, is_up, both(is_up, low_end), both(is_down, high_end)):
        expected = expected + flag.astype(jnp.int32)
    pl.semaphore_wait(barrier, expected - 2 * ring_first.astype(jnp.int32))

    start_sends(0, top, (2,))

    @pl.when(ring_last)
    def _():
        turn_sends(0, 2 * up_rows)

    @pl.when(both(is_last, no(ring_last)))
    def _():
        turn_sends(0, turn_rows)

    @pl.when(no(is_last))
    def _():
        start_sends(0, top, (0,))

    @pl.when(both(is_first, no(ring_first)))
    def _():
        turn_sends(1, turn_rows)

    @pl.when(no(is_first))
    def _():
        start_sends(0, top, (1,))

    for layer in reversed(range(top)):
        for copy in load_copies(layer):
            copy.start()
    acts_copy(0).start()
    goals_copy(0).start()

    @pl.when(ring_last)
    def _():
        pl.semaphore_signal(entry_sem, inc=1, device_id=peers[0], device_id_type=MESH)

    def first_body(idx, carry):
        layer = top - idx
        cast_layer(layer)

        @pl.when(idx == layers // 2)
        def _():
            relay_near()

        @pl.when(idx == (layers + 2) // 2)
        def _():
            relay_far()

        first_sends(layer)
        return carry

    lax.fori_loop(1, layers, first_body, 0)

    @pl.when(ring_first)
    def _():
        pl.semaphore_wait(entry_sem, 1)
        turn_sends(1, 2 * down_rows)

        def late_body(idx, carry):
            start_sends(0, top - idx, (1,))
            return carry

        lax.fori_loop(1, layers, late_body, 0)

    losses[...] = jnp.zeros(losses.shape, F32)

    def step_body(step, carry):
        slot = lax.rem(step, 2)
        later = 1 - slot
        acts_copy(step).wait()

        def forward_body(layer, inner):
            cast_one = copies[slot, layer, :width, :]
            cast_two = copies[slot, layer, width:, :]
            for rows_ds in blocks:
                hid_f = hidden[layer, rows_ds, :].astype(F32)
                inv = lax.rsqrt(jnp.mean(hid_f * hid_f, axis=-1, keepdims=True) + NORM_EPS)
                inv = jnp.broadcast_to(inv, hid_f.shape)
                normed_b = (hid_f * inv).astype(BF16)
                inv_rms[layer, rows_ds, :] = inv
                normed[layer, rows_ds, :] = normed_b
                pre = dot(normed_b, cast_one, 1, 0)
                square = pre * pre
                tanh_v = jnp.tanh(pre * (GELU_SCALE + (GELU_SCALE * GELU_CUBIC) * square))
                cdf = 0.5 + 0.5 * tanh_v
                act_b = (pre * cdf).astype(BF16)
                act[layer, rows_ds, :] = act_b
                inner_slope = 0.5 * GELU_SCALE + (1.5 * GELU_SCALE * GELU_CUBIC) * square
                slope[layer, rows_ds, :] = cdf + (pre * inner_slope) * (1.0 - tanh_v * tanh_v)
                mlp_out = dot(act_b, cast_two, 1, 1)
                hidden[layer + 1, rows_ds, :] = (hid_f + mlp_out).astype(BF16)
            return inner

        lax.fori_loop(0, layers, forward_body, 0)

        @pl.when(step + 1 < steps)
        def _():
            acts_copy(step + 1).start()

        goals_copy(step).wait()
        total = jnp.zeros((8, width), F32)
        for rows_ds in blocks:
            error_term = hidden[layers, rows_ds, :].astype(F32) - goals[rows_ds, :].astype(F32)
            d_hid[rows_ds, :] = (error_term * (2.0 / (rows * width))).astype(BF16)
            total = total + jnp.sum((error_term * error_term).reshape(block // 8, 8, width), axis=0)
        step_loss = jnp.sum(total) / (rows * width)
        lane = lax.broadcasted_iota(jnp.int32, losses.shape, 1)
        losses[...] = jnp.where(lane == step, step_loss, losses[...])

        @pl.when(step + 1 < steps)
        def _():
            goals_copy(step + 1).start()

        def backward_body(idx, inner):
            layer = layers - 1 - idx
            cast_two = copies[slot, layer, width:, :]
            for rows_ds in blocks:
                d_act = dot(d_hid[rows_ds, :], cast_two, 1, 0).astype(BF16).astype(F32)
                d_pre[rows_ds, :] = (d_act * slope[layer, rows_ds, :]).astype(BF16)
            grad_two = dot(d_hid[...], act[layer], 0, 0).astype(BF16)
            grad_one = dot(normed[layer], d_pre[...], 0, 0).astype(BF16)

            is_tail = both(step + 1 == steps, layer == 0)

            @pl.when(no(is_tail))
            def _():
                for copy in sends(slot, layer):
                    copy.wait_recv()

            @pl.when(is_tail)
            def _():
                for copy in tail_half(1):
                    copy.wait_recv()

            @pl.when(step > 0)
            def _():
                for copy in sends(later, layer):
                    copy.wait_send()

            def update(start, grad, master):
                part = pl.ds(start, width)
                other = recv[2, slot, layer, part, :].astype(F32)
                mixed = master[layer] + recv[0, slot, layer, part, :].astype(F32)
                mixed = mixed + recv[1, slot, layer, part, :].astype(F32)
                mixed = mixed + other
                mixed = mixed + other
                fresh = mixed * 0.2 - learn_rate * grad.astype(F32)
                master[layer] = fresh
                copies[later, layer, part, :] = fresh.astype(BF16)

            update(width, grad_two, master_two)

            @pl.when(step + 1 == steps)
            def _():
                stage[layer] = master_two[layer].T

            @pl.when(is_tail)
            def _():
                for copy in tail_half(0):
                    copy.wait_recv()

            update(0, grad_one, master_one)

            @pl.when(layer > 0)
            def _():
                cast_one = copies[slot, layer, :width, :]
                for rows_ds in blocks:
                    d_normed = dot(d_pre[rows_ds, :], cast_one, 1, 1).astype(BF16).astype(F32)
                    inv = inv_rms[layer, rows_ds, :]
                    normed_f = hidden[layer, rows_ds, :].astype(F32) * inv
                    along = jnp.mean(d_normed * normed_f, axis=-1, keepdims=True)
                    d_in = inv * (d_normed - normed_f * along)
                    d_hid[rows_ds, :] = (d_hid[rows_ds, :].astype(F32) + d_in).astype(BF16)

            to_tail = both(step + 2 == steps, layer == 0)

            @pl.when(both(step + 1 < steps, no(to_tail)))
            def _():
                start_sends(later, layer)

            @pl.when(to_tail)
            def _():
                for copy in tail_half(1) + tail_half(0):
                    copy.start()

            return inner

        lax.fori_loop(0, layers, backward_body, 0)
        return carry

    lax.fori_loop(0, steps, step_body, 0)

    def last_body(layer, carry):
        for copy in sends((steps - 1) % 2, layer):
            copy.wait_send()
        return carry

    lax.fori_loop(1, layers, last_body, 0)
    for copy in tail_half(1) + tail_half(0):
        copy.wait_send()

    relay_end()


def write_kernel(one, two, losses, out_one, out_two, out_losses, sems):
    copies = [
        pltpu.make_async_copy(src, dst, sems.at[idx])
        for idx, (src, dst) in enumerate(((one, out_one), (two, out_two), (losses, out_losses)))
    ]
    for copy in copies:
        copy.start()
    for copy in copies:
        copy.wait()


def solution(mesh):
    grid_x = mesh.shape["tx"]

    def device_train(w_one, w_two, inputs, targets):
        layers, width, ffn = w_one.shape[2:]
        steps, rows = inputs.shape[2:4]
        block = min(256, rows)
        dims = (grid_x, steps, layers, rows, width, ffn, block)
        any_spec = pl.BlockSpec(memory_space=pl.ANY)
        vmem_spec = pl.BlockSpec(memory_space=pltpu.VMEM)
        shapes = ((layers, width, ffn), (layers, ffn, width), (1, steps))
        one, two, losses = pl.pallas_call(
            functools.partial(train_kernel, dims),
            out_shape=tuple(pltpu.VMEM(shape, F32) for shape in shapes),
            in_specs=[any_spec] * 4,
            out_specs=(vmem_spec,) * 3,
            scratch_shapes=[
                pltpu.VMEM((layers, width, ffn), F32),
                pltpu.VMEM((2, layers, 2 * width, ffn), BF16),
                pltpu.VMEM((3, 2, layers, 2 * width, ffn), BF16),
                pltpu.VMEM((layers + 1, rows, width), BF16),
                pltpu.VMEM((layers, rows, width), BF16),
                pltpu.VMEM((layers, rows, width), F32),
                pltpu.VMEM((layers, rows, ffn), BF16),
                pltpu.VMEM((layers, rows, ffn), F32),
                pltpu.VMEM((rows, width), BF16),
                pltpu.VMEM((rows, ffn), BF16),
                pltpu.VMEM((rows, width), BF16),
                pltpu.VMEM((2 * width, ffn), BF16),
                pltpu.SemaphoreType.DMA((2, layers)),
                pltpu.SemaphoreType.DMA((2,)),
                pltpu.SemaphoreType.DMA((3, 2, layers)),
                pltpu.SemaphoreType.DMA((3, 2, layers)),
                pltpu.SemaphoreType.DMA((3,)),
                pltpu.SemaphoreType.DMA((2, 3, 2)),
                pltpu.SemaphoreType.REGULAR,
            ],
            compiler_params=pltpu.CompilerParams(
                collective_id=0, has_side_effects=True, vmem_limit_bytes=52 * 1024 * 1024
            ),
            name="gossip_train",
        )(w_one[0, 0], w_two[0, 0], inputs[0, 0], targets[0, 0])
        out_one, out_two, out_losses = pl.pallas_call(
            write_kernel,
            out_shape=tuple(jax.ShapeDtypeStruct(shape, F32) for shape in shapes),
            in_specs=[vmem_spec] * 3,
            out_specs=(any_spec,) * 3,
            scratch_shapes=[pltpu.SemaphoreType.DMA((3,))],
            compiler_params=pltpu.CompilerParams(vmem_limit_bytes=1024 * 1024),
            name="write_out",
        )(one, two, losses)
        return out_one[None, None], out_two[None, None], out_losses[None]

    grid_spec = P("tx", "ty")
    return jax.shard_map(
        device_train,
        mesh=mesh,
        in_specs=(grid_spec, grid_spec, grid_spec, grid_spec),
        out_specs=(grid_spec, grid_spec, grid_spec),
        check_vma=False,
    )
```
